32 devices in a mesh: dp: 8 (over z, y), mp: 4 (over x, core).
Axes of the slice: x: 2, y: 2, z: 4, core: 2. Of those that a mesh axis runs over, the one named last changes fastest.
Arguments:
- pixels: bfloat16 [128, 256, 768], P('dp', 'mp'), may hold values from -6 to 6
- selection: int32 [128], P('dp'), may hold values from 0 to 1, as said below
- destination: int32 [128], P('dp'), may hold values from 0 to 7, as said below
- patch_weight: bfloat16 [768, 1024], replicated, may hold values from -0.21875 to 0.21875
- position: bfloat16 [256, 1024], P('mp'), may hold values from -6 to 6
- query_key_value: bfloat16 [3, 1024, 1024], P(None, None, 'mp'), may hold values from -1 to 1
- output_weight: bfloat16 [1024, 1024], P('mp'), may hold values from -0.1875 to 0.1875
- up_weight: bfloat16 [1024, 4096], P(None, 'mp'), may hold values from -0.1875 to 0.1875
- down_weight: bfloat16 [4096, 1024], P('mp'), may hold values from -0.09375 to 0.09375
- norm_gains: float32 [3, 1024], replicated, may hold values from 0.25 to 1.75
- embedding_weight: bfloat16 [1024, 1024], replicated, may hold values from -0.1875 to 0.1875
- caption_vectors: bfloat16 [128, 1024], P('dp'), may hold values from -6 to 6
- loss_params: float32 [2], replicated, may hold values from -1 to 1
Outputs:
- image_embedding: float32 [32, 1024], P('dp')
- pair_loss: float32 [32], P('dp')
The draws below stay inside these ranges and needn't reach their ends.
Inputs may be any that keep to these rules, and one draw needn't show every extreme that they name: `selection`: exactly 16 examples are selected in all; each index of dp holds between 1 and 3 of them, and some holds exactly 3. Among selected examples, at most 4 have the same destination, some destination has exactly 4, and no index of dp holds two selected examples with the same destination. Destinations of unselected examples are arbitrary.
All inputs are finite; a program needn't handle non-finite values.
Results may differ from the reference program's by a relative error of at most 0.0031.
Values may be sent and summed in bfloat16 or wider, within the bound.
No kernel may reach another device: no remote copies, remote signals or barrier semaphores. Data moves between devices by JAX's collectives and lax.ppermute only.
A program may use at most 128 MiB of HBM per device.

```python
import jax
import jax.numpy as jnp
from jax import lax

D = 1024
HEADS = 16
HEAD_DIM = 64
FF = 4096
PATCHES = 256
EMBED = 1024
PATCH = 768
EX_DEV = 16
SEL_DEV = 2
SEND_MOST = 3
RECV_MOST = 4
EXAMPLES = 128
SELECTED = 16
LEARN_SLOTS = 32
N_DP = 8


def routing_plan(key):
    folded = jax.random.fold_in(key, 11)
    subkeys = jax.random.split(folded, 6)
    halfway = N_DP // 2
    leading = jax.random.randint(subkeys[0], (halfway,), 1, SEND_MOST + 1).at[0].set(SEND_MOST)
    counts = jnp.concatenate([leading, 2 * SEL_DEV - leading])[jax.random.permutation(subkeys[1], N_DP)]
    orders = jax.vmap(lambda subkey: jax.random.permutation(subkey, EX_DEV))(jax.random.split(subkeys[2], N_DP))
    chosen = (orders < counts[:, None]).reshape(EXAMPLES).astype(jnp.int32)
    ranking = jnp.cumsum(chosen) - 1
    load_first = jax.random.randint(subkeys[3], (halfway,), 0, RECV_MOST + 1).at[0].set(RECV_MOST)
    receiver_loads = jnp.concatenate([load_first, 2 * SEL_DEV - load_first])[jax.random.permutation(subkeys[4], N_DP)]
    boundaries = jnp.cumsum(receiver_loads)
    stride = SELECTED // RECV_MOST
    places = ranking % stride * RECV_MOST + ranking // stride
    listed = jnp.sum((boundaries[None, :] <= places[:, None]).astype(jnp.int32), axis=1)
    filler = jax.random.randint(subkeys[5], (EXAMPLES,), 0, N_DP)
    targets = jnp.where(chosen > 0, listed, filler).astype(jnp.int32)
    return (chosen, targets)


def draw_selection(key, part):
    return routing_plan(key)[0]


def draw_destination(key, part):
    return routing_plan(key)[1]


def draw_query_key_value(key, part):
    folded = jax.random.fold_in(key, 23)
    subkeys = jax.random.split(folded, 1)
    values = jax.random.normal(subkeys[0], (3, D, D), jnp.float32) * D ** (-0.5)
    return jnp.clip(values, -1.0, 1.0).astype(jnp.bfloat16)


def steps_of(key, extent, cuts, least, high):
    loudness, own = 1.0, jax.random.fold_in(key, 6)
    for dim, shards_of in cuts:
        heights = jnp.exp(jax.random.uniform(jax.random.fold_in(own, dim), (shards_of,), jnp.float32, least / len(cuts), high / len(cuts)))
        loudness = loudness * jnp.repeat(heights, extent[dim] // shards_of).reshape([-1 if axis == dim else 1 for axis in range(len(extent))])
    return loudness


def normal_values(stream_key, dims, scale, limit, cuts=(), kind=jnp.bfloat16):
    array = scale * jax.random.normal(stream_key, dims, jnp.float32)
    if cuts:
        array = array * steps_of(stream_key, dims, cuts, -0.22, 0.18)
    return jnp.clip(array, -limit, limit).astype(kind)


def setup_inputs(seed: int = 0) -> dict:
    key_list = jax.random.split(jax.random.key(seed), 14)
    return {
        "pixels": normal_values(key_list[0], (EXAMPLES, PATCHES, PATCH), 1.0, 6.0, ((0, 8), (1, 4))),
        "selection": draw_selection(jax.random.fold_in(key_list[13], 71), 0),
        "destination": draw_destination(jax.random.fold_in(key_list[13], 71), 0),
        "patch_weight": normal_values(key_list[3], (PATCH, D), PATCH ** -0.5, 0.21875),
        "position": normal_values(key_list[4], (PATCHES, D), 1.0, 6.0, ((0, 4),)),
        "query_key_value": draw_query_key_value(jax.random.fold_in(key_list[13], 71), 0),
        "output_weight": normal_values(key_list[6], (D, D), D ** -0.5, 0.1875, ((0, 4),)),
        "up_weight": normal_values(key_list[7], (D, FF), D ** -0.5, 0.1875, ((1, 4),)),
        "down_weight": normal_values(key_list[8], (FF, D), FF ** -0.5, 0.09375, ((0, 4),)),
        "norm_gains": jnp.clip(1.0 + 0.15 * jax.random.normal(key_list[9], (3, D), jnp.float32), 0.25, 1.75),
        "embedding_weight": normal_values(key_list[10], (D, EMBED), D ** -0.5, 0.1875),
        "caption_vectors": normal_values(key_list[11], (EXAMPLES, EMBED), 1.0, 6.0, ((0, 8),)),
        "loss_params": jnp.clip(jax.random.uniform(key_list[12], (2,), jnp.float32, -1.0, 1.0), -1.0, 1.0),
    }


EPS = 1e-06

def layer_norm(values, gain):
    center = lax.optimization_barrier(jnp.mean(values, axis=-1, keepdims=True))
    centred = values - center
    spread = lax.optimization_barrier(jnp.mean(centred * centred, axis=-1, keepdims=True))
    return centred * lax.rsqrt(spread + EPS) * gain.astype(jnp.float32)

def unit_rows(values):
    scale = lax.rsqrt(lax.optimization_barrier(jnp.mean(values * values, axis=-1, keepdims=True)) + EPS)
    return values * scale * values.shape[-1] ** (-0.5)

def encode_image(image, patch_weight, position, qkv_flat, output_weight, up_weight, down_weight, norm_gains):
    hidden = jnp.dot(image, patch_weight, preferred_element_type=jnp.float32) + position.astype(jnp.float32)
    normed = layer_norm(hidden, norm_gains[0]).astype(jnp.bfloat16)
    projected = jnp.dot(normed, qkv_flat, preferred_element_type=jnp.float32).astype(jnp.bfloat16)
    shaped = projected.reshape(PATCHES, 3, HEADS, HEAD_DIM).astype(jnp.float32)
    query_rows = shaped[:, 0]
    key_rows = shaped[:, 1]
    value_rows = shaped[:, 2]
    scores = jnp.einsum('qhd,khd->hqk', query_rows, key_rows) * HEAD_DIM ** (-0.5)
    weights = jax.nn.softmax(scores, axis=-1).astype(jnp.bfloat16)
    context = jnp.einsum('hqk,khd->qhd', weights.astype(jnp.float32), value_rows).astype(jnp.bfloat16)
    context = context.reshape(PATCHES, D)
    hidden = hidden + jnp.dot(context, output_weight, preferred_element_type=jnp.float32)
    normed = layer_norm(hidden, norm_gains[1]).astype(jnp.bfloat16)
    expanded = jax.nn.gelu(jnp.dot(normed, up_weight, preferred_element_type=jnp.float32)).astype(jnp.bfloat16)
    hidden = hidden + jnp.dot(expanded, down_weight, preferred_element_type=jnp.float32)
    return lax.optimization_barrier(jnp.mean(hidden, axis=0))

def pair_terms(embedded, slot_example, texts, text_ids, text_live, loss_params, live, total):
    images = unit_rows(embedded)
    captions = unit_rows(texts)
    scale = 10.0 * jnp.exp(loss_params[0])
    shift = 2.0 * loss_params[1]
    logits = scale * jnp.dot(images, captions.T, precision=lax.Precision.HIGHEST) + shift
    signs = jnp.where(slot_example[:, None] == text_ids[None, :], 1.0, -1.0).astype(jnp.float32)
    terms = jax.nn.softplus(-signs * logits) * text_live[None, :].astype(jnp.float32)
    return jnp.where(live, lax.optimization_barrier(jnp.sum(terms, axis=1)) / total, 0.0).astype(jnp.float32)

def reference(pixels, selection, destination, patch_weight, position, query_key_value, output_weight, up_weight, down_weight, norm_gains, embedding_weight, caption_vectors, loss_params):
    indices = jnp.arange(EXAMPLES, dtype=jnp.int32)
    chosen = selection > 0
    ranking = (jnp.cumsum(selection) - 1).astype(jnp.int32)
    ordered = jnp.zeros((SELECTED,), jnp.int32).at[jnp.where(chosen, ranking, SELECTED).astype(jnp.int32)].set(indices, mode='drop')
    qkv_flat = query_key_value.transpose(1, 0, 2).reshape(D, 3 * D)

    def encode_one(example):
        return encode_image(pixels[example], patch_weight, position, qkv_flat, output_weight, up_weight, down_weight, norm_gains)
    pooled_list = lax.map(encode_one, ordered)
    hot = ((destination[:, None] == jnp.arange(N_DP, dtype=jnp.int32)[None, :]) & chosen[:, None]).astype(jnp.int32)
    running = jnp.cumsum(hot, axis=0)
    within = (lax.optimization_barrier(jnp.sum(running * hot, axis=1)) - 1).astype(jnp.int32)
    flat_slot = jnp.where(chosen, destination * RECV_MOST + within, LEARN_SLOTS).astype(jnp.int32)
    slot_rank = jnp.full((LEARN_SLOTS,), -1, jnp.int32).at[flat_slot].set(ranking, mode='drop')
    live = slot_rank >= 0
    safe_rank = jnp.maximum(slot_rank, 0).astype(jnp.int32)
    pooled = pooled_list[safe_rank]
    slot_example = jnp.where(live, ordered[safe_rank], -1).astype(jnp.int32)
    normed = layer_norm(pooled, norm_gains[2]).astype(jnp.bfloat16)
    embedded = jnp.dot(normed, embedding_weight, preferred_element_type=jnp.float32)
    embedded = jnp.where(live[:, None], embedded, 0.0).astype(jnp.float32)
    texts = caption_vectors[ordered].astype(jnp.float32)
    text_live = jnp.ones((SELECTED,), dtype=bool)
    losses = pair_terms(embedded, slot_example, texts, ordered, text_live, loss_params, live, float(SELECTED))
    return (embedded, losses)
```

```python
import functools

import jax
import jax.numpy as jnp
from jax import lax
from jax.experimental import pallas as pl
from jax.experimental.pallas import tpu as pltpu
from jax.sharding import PartitionSpec as P

HEAD_DIM = 64
SEL_DEV = 2
SEND_MOST = 3
RECV_MOST = 4
META = 128
EPS = 1e-06

VMEM = pltpu.MemorySpace.VMEM
SMEM = pltpu.MemorySpace.SMEM
F32 = jnp.float32
BF16 = jnp.bfloat16


def vmem():
    return pl.BlockSpec(memory_space=VMEM)


def smem():
    return pl.BlockSpec(memory_space=SMEM)


def layer_norm(values, gain):
    center = jnp.mean(values, axis=-1, keepdims=True)
    centred = values - center
    spread = jnp.mean(centred * centred, axis=-1, keepdims=True)
    return centred * lax.rsqrt(spread + EPS) * gain


def unit_rows(values):
    scale = lax.rsqrt(jnp.mean(values * values, axis=-1, keepdims=True) + EPS)
    return values * scale * values.shape[-1] ** (-0.5)


def swap(values, axis, bit):
    size = lax.axis_size(axis)
    return lax.ppermute(values, axis, [(i, i ^ bit) for i in range(size)])


def bits_down(size):
    bits = []
    bit = size // 2
    while bit:
        bits.append(bit)
        bit //= 2
    return bits


def gather_blocks(values, axis):
    blocks, order = [values], [0]
    for bit in bits_down(lax.axis_size(axis)):
        blocks = blocks + [swap(block, axis, bit) for block in blocks]
        order = order + [other ^ bit for other in order]
    return blocks, order


def double_stack(values, axis):
    stacked = values[None]
    bit = 1
    while bit < lax.axis_size(axis):
        stacked = jnp.concatenate([stacked, swap(stacked, axis, bit)], axis=0)
        bit *= 2
    return stacked


def pick_kernel(sel_ref, dest_ref, pixels_ref, cap_ref, rows_ref, meta_ref, sems):
    count = jnp.int32(0)
    index = [jnp.int32(0)] * SEND_MOST
    target = [jnp.int32(0)] * SEND_MOST
    for e in range(sel_ref.shape[0]):
        here = sel_ref[e] > 0
        for r in range(SEND_MOST):
            take = here & (count == r)
            index[r] = jnp.where(take, e, index[r])
            target[r] = jnp.where(take, dest_ref[e], target[r])
        count = count + here.astype(jnp.int32)
    copies = []
    for r in range(SEND_MOST):
        copies.append(
            pltpu.make_async_copy(pixels_ref.at[index[r]], rows_ref.at[r], sems.at[r])
        )
        copies[-1].start()
    captions = cap_ref[...].astype(F32)
    width = captions.shape[1]
    example = lax.broadcasted_iota(jnp.int32, captions.shape, 0)
    lane = lax.broadcasted_iota(jnp.int32, (1, META), 1)
    for r in range(SEND_MOST):
        row = jnp.sum(jnp.where(example == index[r], captions, 0.0), axis=0, keepdims=True)
        live = (count > r).astype(F32)
        extra = jnp.where(lane == 0, live, jnp.where(lane == 1, target[r].astype(F32), 0.0))
        meta_ref[r : r + 1, :width] = row.astype(BF16)
        meta_ref[r : r + 1, width:] = extra.astype(BF16)
    for copy in copies:
        copy.wait()


def pick(selection, destination, pixels, captions):
    _, length, depth = pixels.shape
    return pl.pallas_call(
        pick_kernel,
        out_shape=(
            jax.ShapeDtypeStruct((SEND_MOST, length, depth), BF16),
            jax.ShapeDtypeStruct((SEND_MOST, captions.shape[1] + META), BF16),
        ),
        in_specs=[smem(), smem(), pl.BlockSpec(memory_space=pl.ANY), vmem()],
        out_specs=(vmem(), vmem()),
        scratch_shapes=[pltpu.SemaphoreType.DMA((SEND_MOST,))],
        name="pick",
    )(selection, destination, pixels, captions)


def attend_kernel(shards, gains_ref, patch_ref, qkv_ref, *refs):
    pixel_refs = refs[:shards]
    position_refs = refs[shards : 2 * shards]
    hidden_ref, context_ref = refs[2 * shards :]
    pixels = jnp.concatenate([ref[...] for ref in pixel_refs], axis=0)
    position = jnp.concatenate([ref[...] for ref in position_refs], axis=0)
    hidden = jnp.dot(pixels, patch_ref[...], preferred_element_type=F32)
    hidden = hidden + position.astype(F32)
    hidden_ref[...] = hidden
    normed = layer_norm(hidden, gains_ref[0:1, :]).astype(BF16)
    query, key, value = [
        jnp.dot(normed, qkv_ref[t], preferred_element_type=F32).astype(BF16) for t in range(3)
    ]
    query = query * jnp.asarray(HEAD_DIM ** (-0.5), BF16)
    parts = []
    for h in range(query.shape[1] // HEAD_DIM):
        cols = slice(h * HEAD_DIM, (h + 1) * HEAD_DIM)
        scores = lax.dot_general(
            query[:, cols], key[:, cols], (((1,), (1,)), ((), ())), preferred_element_type=F32
        )
        weights = jnp.exp(scores - jnp.max(scores, axis=-1, keepdims=True))
        weights = weights * (1.0 / jnp.sum(weights, axis=-1, keepdims=True))
        parts.append(jnp.dot(weights.astype(BF16), value[:, cols], preferred_element_type=F32))
    context_ref[...] = jnp.concatenate(parts, axis=1).astype(BF16)


def attend(pixels, positions, gains, patch_weight, qkv):
    shards = len(pixels)
    length = shards * pixels[0].shape[0]
    width = patch_weight.shape[1]
    return pl.pallas_call(
        functools.partial(attend_kernel, shards),
        out_shape=(
            jax.ShapeDtypeStruct((length, width), F32),
            jax.ShapeDtypeStruct((length, qkv.shape[2]), BF16),
        ),
        in_specs=[vmem()] * (3 + 2 * shards),
        out_specs=(vmem(), vmem()),
        name="attend",
    )(gains, patch_weight, qkv, *pixels, *positions)


def expand_kernel(order, gains_ref, up_ref, hidden_ref, *refs):
    shards = len(order)
    context_refs = refs[:shards]
    output_refs = refs[shards : 2 * shards]
    sums_ref = refs[2 * shards]
    block = hidden_ref.shape[0] // shards
    hidden = hidden_ref[...]
    for j, ref in enumerate(context_refs):
        places = [order.index(order[p] ^ order[j]) for p in range(shards)]
        context = jnp.concatenate([ref[q * block : (q + 1) * block, :] for q in places], axis=0)
        hidden = hidden + jnp.dot(context, output_refs[j][...], preferred_element_type=F32)
    normed = layer_norm(hidden, gains_ref[1:2, :]).astype(BF16)
    expanded = jax.nn.gelu(jnp.dot(normed, up_ref[...], preferred_element_type=F32)).astype(BF16)
    sums_ref[0:1, :] = jnp.sum(hidden, axis=0, keepdims=True)
    sums_ref[1:2, :] = jnp.sum(expanded.astype(F32), axis=0, keepdims=True)


def expand(contexts, order, outputs, hidden, gains, up_weight):
    width = hidden.shape[1]
    return pl.pallas_call(
        functools.partial(expand_kernel, tuple(order)),
        out_shape=jax.ShapeDtypeStruct((2, width), F32),
        in_specs=[vmem()] * (3 + 2 * len(order)),
        out_specs=vmem(),
        name="expand",
    )(gains, up_weight, hidden, *contexts, *outputs)


def reduce_kernel(scale, own_ref, down_ref, *refs):
    out_ref = refs[-1]
    sums = refs[:-1]
    units = jnp.concatenate([ref[1:2, :] for ref in sums], axis=0) * scale
    residual = jnp.concatenate([ref[0:1, :] for ref in sums], axis=0) * scale
    high = units.astype(BF16)
    low = (units - high.astype(F32)).astype(BF16)
    both = jnp.concatenate([high, low], axis=0)
    product = jnp.dot(both, down_ref[...], preferred_element_type=F32)
    count = len(sums)
    own = own_ref[0].astype(F32)
    out_ref[...] = product[:count] + product[count:] + residual * own


def reduce_units(sums, own, down_weight, patches):
    return pl.pallas_call(
        functools.partial(reduce_kernel, 1.0 / patches),
        out_shape=jax.ShapeDtypeStruct((len(sums), down_weight.shape[1]), F32),
        in_specs=[smem()] + [vmem()] * (1 + len(sums)),
        out_specs=vmem(),
        name="reduce",
    )(own, down_weight, *sums)


def finish_kernel(total, params_ref, gains_ref, weight_ref, cap_ref, meta_ref, pooled_ref, out_ref, loss_ref):
    count = meta_ref.shape[0]
    rows = [
        pooled_ref[c // SEND_MOST, c % SEND_MOST : c % SEND_MOST + 1, :] for c in range(count)
    ]
    meta = meta_ref[...]
    live = meta[:, 0:1]
    slots = []
    for k in range(RECV_MOST):
        acc = None
        for c in range(count):
            term = jnp.where(meta[c : c + 1, k + 1 : k + 2] > 0.0, rows[c], 0.0)
            acc = term if acc is None else acc + term
        slots.append(acc)
    pooled = jnp.concatenate(slots, axis=0)
    filled = jnp.max(meta[:, 1 : RECV_MOST + 1], axis=0, keepdims=True)
    normed = layer_norm(pooled, gains_ref[2:3, :]).astype(BF16)
    embedded = jnp.dot(normed, weight_ref[...], preferred_element_type=F32)
    captions = cap_ref[...]
    scale = 10.0 * jnp.exp(jnp.full((1, 1), params_ref[0], F32))
    shift = 2.0 * params_ref[1]
    for k in range(RECV_MOST):
        used = filled[:, k : k + 1] > 0.0
        row = jnp.where(used, embedded[k : k + 1, :], 0.0)
        out_ref[k : k + 1, :] = row
        logits = scale * jnp.sum(captions * unit_rows(row), axis=1, keepdims=True) + shift
        signs = jnp.where(meta[:, k + 1 : k + 2] > 0.0, 1.0, -1.0)
        value = -signs * logits
        terms = jnp.maximum(value, 0.0) + jnp.log1p(jnp.exp(-jnp.abs(value)))
        lost = jnp.sum(terms * live) / total
        loss_ref[k] = jnp.where(jnp.max(jnp.where(used, 1.0, 0.0)) > 0.0, lost, 0.0)


def finish(pooled, captions, meta, params, gains, weight, total):
    return pl.pallas_call(
        functools.partial(finish_kernel, total),
        out_shape=(
            jax.ShapeDtypeStruct((RECV_MOST, weight.shape[1]), F32),
            jax.ShapeDtypeStruct((RECV_MOST,), F32),
        ),
        in_specs=[smem()] + [vmem()] * 5,
        out_specs=(vmem(), smem()),
        name="finish",
    )(params, gains, weight, captions, meta, pooled)


def per_device(
    pixels,
    selection,
    destination,
    patch_weight,
    position,
    query_key_value,
    output_weight,
    up_weight,
    down_weight,
    norm_gains,
    embedding_weight,
    caption_vectors,
    loss_params,
):
    devices_dp = lax.axis_size("dp")
    rows, caption_meta = pick(selection, destination, pixels, caption_vectors)
    positions, order = gather_blocks(position, "mp")
    pixel_blocks = [gather_blocks(rows[r], "mp")[0] for r in range(SEND_MOST)]
    outputs, _ = gather_blocks(output_weight, "mp")

    me = lax.axis_index("dp")
    width = caption_vectors.shape[1]
    gathered = double_stack(caption_meta, "dp").reshape(devices_dp * SEND_MOST, width + META)
    captions = unit_rows(gathered[:, :width].astype(F32))
    live = gathered[:, width] > 0
    target = gathered[:, width + 1].astype(jnp.int32)
    spot = (me ^ jnp.arange(devices_dp, dtype=jnp.int32))[:, None] * SEND_MOST
    spot = (spot + jnp.arange(SEND_MOST, dtype=jnp.int32)).reshape(-1)
    mine = live & (target == me)
    ahead = mine[None, :] & (spot[None, :] < spot[:, None])
    place = jnp.sum(ahead.astype(jnp.int32), axis=1)
    slot = mine[:, None] & (place[:, None] == jnp.arange(RECV_MOST, dtype=jnp.int32))
    meta = jnp.concatenate([live[:, None], slot], axis=1).astype(F32)

    sums = []
    for r in range(SEND_MOST):
        hidden, context = attend(pixel_blocks[r], positions, norm_gains, patch_weight, query_key_value)
        contexts, _ = gather_blocks(context, "mp")
        sums.append(expand(contexts, order, outputs, hidden, norm_gains, up_weight))
    own = (lax.axis_index("mp") == 0).astype(jnp.int32).reshape(1)
    patches = position.shape[0] * len(order)
    pooled = reduce_units(sums, own, down_weight, patches)
    for bit in reversed(bits_down(lax.axis_size("mp"))):
        pooled = pooled + swap(pooled, "mp", bit)
    pooled = double_stack(pooled, "dp")
    return finish(
        pooled, captions, meta, loss_params, norm_gains, embedding_weight, float(devices_dp * SEL_DEV)
    )


def solution(mesh):
    in_specs = (
        P("dp", "mp", None),
        P("dp"),
        P("dp"),
        P(),
        P("mp", None),
        P(None, None, "mp"),
        P("mp", None),
        P(None, "mp"),
        P("mp", None),
        P(),
        P(),
        P("dp", None),
        P(),
    )
    out_specs = (P("dp", None), P("dp"))
    return jax.shard_map(
        per_device, mesh=mesh, in_specs=in_specs, out_specs=out_specs, check_vma=False
    )
```

```python
import functools

import jax
import jax.numpy as jnp
from jax import lax
from jax.experimental import pallas as pl
from jax.experimental.pallas import tpu as pltpu
from jax.sharding import PartitionSpec as P


HEAD_DIM = 64
SEL_DEV = 2
SEND_MOST = 3
RECV_MOST = 4
META = 128
PIECES = 2
EPS = 1e-06


VMEM = pltpu.MemorySpace.VMEM
SMEM = pltpu.MemorySpace.SMEM
F32 = jnp.float32
BF16 = jnp.bfloat16


def vmem():
    return pl.BlockSpec(memory_space=VMEM)


def smem():
    return pl.BlockSpec(memory_space=SMEM)


def layer_norm(values, gain):
    center = jnp.mean(values, axis=-1, keepdims=True)
    centred = values - center
    spread = jnp.mean(centred * centred, axis=-1, keepdims=True)
    return centred * lax.rsqrt(spread + EPS) * gain


def unit_rows(values):
    scale = lax.rsqrt(jnp.mean(values * values, axis=-1, keepdims=True) + EPS)
    return values * scale * values.shape[-1] ** (-0.5)


def swap(values, axis, bit):
    size = lax.axis_size(axis)
    return lax.ppermute(values, axis, [(i, i ^ bit) for i in range(size)])


def bits_down(size):
    bits = []
    bit = size // 2
    while bit:
        bits.append(bit)
        bit //= 2
    return bits


def gather_blocks(values, axis):
    blocks, order = [values], [0]
    for bit in bits_down(lax.axis_size(axis)):
        blocks = blocks + [swap(block, axis, bit) for block in blocks]
        order = order + [other ^ bit for other in order]
    return blocks, order


def small(mib):
    return pltpu.CompilerParams(vmem_limit_bytes=mib << 20)


def join_kernel(own_ref, other_ref, out_ref):
    count = own_ref.shape[0]
    out_ref[:count] = own_ref[...]
    out_ref[count:] = other_ref[...]


def join(own, other):
    return pl.pallas_call(
        join_kernel,
        out_shape=jax.ShapeDtypeStruct((2 * own.shape[0],) + own.shape[1:], own.dtype),
        in_specs=[vmem()] * 2,
        out_specs=vmem(),
        compiler_params=small(2),
    )(own, other)


def add_kernel(own_ref, other_ref, out_ref):
    out_ref[...] = own_ref[...] + other_ref[...]


def add(own, other):
    return pl.pallas_call(
        add_kernel,
        out_shape=jax.ShapeDtypeStruct(own.shape, own.dtype),
        in_specs=[vmem()] * 2,
        out_specs=vmem(),
        name="add",
        compiler_params=small(1),
    )(own, other)


def double_stack(values, axis):
    size = lax.axis_size(axis)
    bit = 1
    while 2 * bit < size:
        values = join(values, swap(values, axis, bit))
        bit *= 2
    return values, swap(values, axis, bit)


def pick_kernel(pieces, sel_hbm, dest_hbm, pixels_ref, cap_hbm, output_ref, *refs):
    row_refs = refs[:SEND_MOST]
    meta_ref, piece_ref, sel_ref, dest_ref, cap_ref, sems = refs[SEND_MOST:]
    first = [
        pltpu.make_async_copy(source, target, sems.at[SEND_MOST + 1 + i])
        for i, (source, target) in enumerate(
            ((sel_hbm, sel_ref), (dest_hbm, dest_ref), (cap_hbm, cap_ref))
        )
    ]
    for copy in first:
        copy.start()
    first[0].wait()
    first[1].wait()
    count = jnp.int32(0)
    index = [jnp.int32(0)] * SEND_MOST
    target = [jnp.int32(0)] * SEND_MOST
    for e in range(sel_ref.shape[0]):
        here = sel_ref[e] > 0
        for r in range(SEND_MOST):
            take = here & (count == r)
            index[r] = jnp.where(take, e, index[r])
            target[r] = jnp.where(take, dest_ref[e], target[r])
        count = count + here.astype(jnp.int32)
    copies = [
        pltpu.make_async_copy(pixels_ref.at[index[r]], row_refs[r], sems.at[r])
        for r in range(SEND_MOST)
    ]
    height = piece_ref.shape[0]
    start = pl.multiple_of((lax.axis_index("dp") & (pieces - 1)) * height, height)
    copies.append(
        pltpu.make_async_copy(output_ref.at[pl.ds(start, height)], piece_ref, sems.at[SEND_MOST])
    )
    for copy in copies:
        copy.start()
    first[2].wait()
    captions = cap_ref[...].astype(F32)
    width = captions.shape[1]
    example = lax.broadcasted_iota(jnp.int32, captions.shape, 0)
    lane = lax.broadcasted_iota(jnp.int32, (1, META), 1)
    for r in range(SEND_MOST):
        row = jnp.sum(jnp.where(example == index[r], captions, 0.0), axis=0, keepdims=True)
        live = (count > r).astype(F32)
        extra = jnp.where(lane == 0, live, jnp.where(lane == 1, target[r].astype(F32), 0.0))
        meta_ref[0, r : r + 1, :width] = row.astype(BF16)
        meta_ref[0, r : r + 1, width:] = extra.astype(BF16)
    for copy in copies:
        copy.wait()


def pick(selection, destination, pixels, captions, output_weight, pieces):
    _, length, depth = pixels.shape
    fan, width = output_weight.shape
    hbm = pl.BlockSpec(memory_space=pltpu.MemorySpace.HBM)
    *rows, caption_meta, piece = pl.pallas_call(
        functools.partial(pick_kernel, pieces),
        out_shape=(jax.ShapeDtypeStruct((length, depth), BF16),) * SEND_MOST
        + (
            jax.ShapeDtypeStruct((1, SEND_MOST, captions.shape[1] + META), BF16),
            jax.ShapeDtypeStruct((fan // pieces, width), BF16),
        ),
        in_specs=[hbm] * 5,
        out_specs=(vmem(),) * (SEND_MOST + 2),
        scratch_shapes=[
            SMEM(selection.shape, jnp.int32),
            SMEM(destination.shape, jnp.int32),
            VMEM(captions.shape, BF16),
            pltpu.SemaphoreType.DMA((SEND_MOST + 4,)),
        ],
        name="pick",
        compiler_params=small(2),
    )(*(
        pltpu.with_memory_space_constraint(array, pltpu.MemorySpace.HBM)
        for array in (selection, destination, pixels, captions, output_weight)
    ))
    return rows, caption_meta, piece


def assemble_kernel(*refs):
    out_ref = refs[-1]
    pieces = refs[:-1]
    height = pieces[0].shape[0]
    here = lax.axis_index("dp") & (len(pieces) - 1)
    for j, ref in enumerate(pieces):
        start = pl.multiple_of((here ^ j) * height, height)
        out_ref[pl.ds(start, height), :] = ref[...]


def assemble(pieces):
    height, width = pieces[0].shape
    return pl.pallas_call(
        assemble_kernel,
        out_shape=jax.ShapeDtypeStruct((height * len(pieces), width), BF16),
        in_specs=[vmem()] * len(pieces),
        out_specs=vmem(),
        name="assemble",
        compiler_params=small(2),
    )(*pieces)


def route_kernel(first_ref, second_ref, cap_ref, meta_ref):
    half = first_ref.shape[0]
    rows = jnp.concatenate(
        [ref[j].astype(F32) for ref in (first_ref, second_ref) for j in range(half)], axis=0
    )
    width = cap_ref.shape[1]
    cap_ref[...] = unit_rows(rows[:, :width])
    extra = rows[:, width:]
    live, target = extra[:, 0:1], extra[:, 1:2]
    me = lax.axis_index("dp")
    offset = lax.broadcasted_iota(jnp.int32, (SEND_MOST, 1), 0)
    spot = jnp.concatenate([(me ^ j) * SEND_MOST + offset for j in range(2 * half)], axis=0)
    mine = (live > 0.0) & (target == me.astype(F32))
    mine = jnp.where(mine, 1.0, 0.0)
    count = rows.shape[0]
    square = (count, count)
    same = lax.broadcasted_iota(jnp.int32, square, 0) == lax.broadcasted_iota(jnp.int32, square, 1)
    mine_row = jnp.sum(jnp.where(same, mine, 0.0), axis=0, keepdims=True)
    spot_col = spot.astype(F32)
    spot_row = jnp.sum(jnp.where(same, spot_col, 0.0), axis=0, keepdims=True)
    place = jnp.sum(jnp.where(spot_row < spot_col, mine_row, 0.0), axis=1, keepdims=True)
    lane = lax.broadcasted_iota(jnp.int32, (count, META), 1)
    slot = jnp.where(place == (lane - 1).astype(F32), mine, 0.0)
    meta_ref[...] = jnp.where(lane == 0, live, slot)


def route(first, second):
    count = 2 * first.shape[0] * SEND_MOST
    return pl.pallas_call(
        route_kernel,
        out_shape=(
            jax.ShapeDtypeStruct((count, first.shape[2] - META), F32),
            jax.ShapeDtypeStruct((count, META), F32),
        ),
        in_specs=[vmem()] * 2,
        out_specs=(vmem(),) * 2,
        name="route",
        compiler_params=small(6),
    )(first, second)


def attend_kernel(shards, gains_ref, patch_ref, qkv_ref, *refs):
    pixel_refs = refs[:shards]
    position_refs = refs[shards : 2 * shards]
    hidden_ref, context_ref = refs[2 * shards :]
    pixels = jnp.concatenate([ref[...] for ref in pixel_refs], axis=0)
    position = jnp.concatenate([ref[...] for ref in position_refs], axis=0)
    hidden = jnp.dot(pixels, patch_ref[...], preferred_element_type=F32)
    hidden = hidden + position.astype(F32)
    hidden_ref[...] = hidden
    normed = layer_norm(hidden, gains_ref[0:1, :]).astype(BF16)
    query, key, value = [
        jnp.dot(normed, qkv_ref[t], preferred_element_type=F32).astype(BF16) for t in range(3)
    ]
    query = query * jnp.asarray(HEAD_DIM ** (-0.5), BF16)
    parts = []
    for h in range(query.shape[1] // HEAD_DIM):
        cols = slice(h * HEAD_DIM, (h + 1) * HEAD_DIM)
        scores = lax.dot_general(
            query[:, cols], key[:, cols], (((1,), (1,)), ((), ())), preferred_element_type=F32
        )
        weights = jnp.exp(scores - jnp.max(scores, axis=-1, keepdims=True))
        weights = weights * (1.0 / jnp.sum(weights, axis=-1, keepdims=True))
        parts.append(jnp.dot(weights.astype(BF16), value[:, cols], preferred_element_type=F32))
    context_ref[...] = jnp.concatenate(parts, axis=1).astype(BF16)


def attend(pixels, positions, gains, patch_weight, qkv):
    shards = len(pixels)
    length = shards * pixels[0].shape[0]
    width = patch_weight.shape[1]
    return pl.pallas_call(
        functools.partial(attend_kernel, shards),
        out_shape=(
            jax.ShapeDtypeStruct((length, width), F32),
            jax.ShapeDtypeStruct((length, qkv.shape[2]), BF16),
        ),
        in_specs=[vmem()] * (3 + 2 * shards),
        out_specs=(vmem(), vmem()),
        compiler_params=small(14),
    )(gains, patch_weight, qkv, *pixels, *positions)


def expand_kernel(order, gains_ref, up_ref, hidden_ref, *refs):
    shards = len(order)
    context_refs = refs[:shards]
    output_refs = refs[shards : 2 * shards]
    sums_ref = refs[2 * shards]
    block = hidden_ref.shape[0] // shards
    hidden = hidden_ref[...]
    for j, ref in enumerate(context_refs):
        places = [order.index(order[p] ^ order[j]) for p in range(shards)]
        context = jnp.concatenate([ref[q * block : (q + 1) * block, :] for q in places], axis=0)
        hidden = hidden + jnp.dot(context, output_refs[j][...], preferred_element_type=F32)
    normed = layer_norm(hidden, gains_ref[1:2, :]).astype(BF16)
    expanded = jax.nn.gelu(jnp.dot(normed, up_ref[...], preferred_element_type=F32)).astype(BF16)
    sums_ref[0:1, :] = jnp.sum(hidden, axis=0, keepdims=True)
    sums_ref[1:2, :] = jnp.sum(expanded.astype(F32), axis=0, keepdims=True)


def expand(contexts, order, outputs, hidden, gains, up_weight):
    width = hidden.shape[1]
    return pl.pallas_call(
        functools.partial(expand_kernel, tuple(order)),
        out_shape=jax.ShapeDtypeStruct((2, width), F32),
        in_specs=[vmem()] * (3 + 2 * len(order)),
        out_specs=vmem(),
        compiler_params=small(14),
    )(gains, up_weight, hidden, *contexts, *outputs)


def reduce_kernel(scale, down_ref, *refs):
    out_ref = refs[-1]
    sums = refs[:-1]
    units = jnp.concatenate([ref[1:2, :] for ref in sums], axis=0) * scale
    residual = jnp.concatenate([ref[0:1, :] for ref in sums], axis=0) * scale
    high = units.astype(BF16)
    low = (units - high.astype(F32)).astype(BF16)
    both = jnp.concatenate([high, low], axis=0)
    product = jnp.dot(both, down_ref[...], preferred_element_type=F32)
    count = len(sums)
    own = (lax.axis_index("mp") == 0).astype(F32)
    out_ref[...] = product[:count] + product[count:] + residual * own


def reduce_units(sums, down_weight, patches):
    return pl.pallas_call(
        functools.partial(reduce_kernel, 1.0 / patches),
        out_shape=jax.ShapeDtypeStruct((len(sums), down_weight.shape[1]), F32),
        in_specs=[vmem()] * (1 + len(sums)),
        out_specs=vmem(),
        name="reduce",
        compiler_params=small(6),
    )(down_weight, *sums)


def finish_kernel(total, params_ref, gains_ref, weight_ref, cap_ref, meta_ref, first_ref, second_ref, out_ref, loss_ref):
    half = first_ref.shape[0]
    rows = jnp.concatenate(
        [ref[j] for ref in (first_ref, second_ref) for j in range(half)], axis=0
    )
    meta = meta_ref[...]
    live = meta[:, 0:1]
    pooled = jnp.concatenate(
        [
            jnp.sum(jnp.where(meta[:, k + 1 : k + 2] > 0.0, rows, 0.0), axis=0, keepdims=True)
            for k in range(RECV_MOST)
        ],
        axis=0,
    )
    filled = jnp.max(meta, axis=0, keepdims=True)
    normed = layer_norm(pooled, gains_ref[2:3, :]).astype(BF16)
    embedded = jnp.dot(normed, weight_ref[...], preferred_element_type=F32)
    captions = cap_ref[...]
    scale = 10.0 * jnp.exp(jnp.full((1, 1), params_ref[0], F32))
    shift = 2.0 * params_ref[1]
    for k in range(RECV_MOST):
        used = filled[:, k + 1 : k + 2]
        row = jnp.where(used > 0.0, embedded[k : k + 1, :], 0.0)
        out_ref[k : k + 1, :] = row
        logits = scale * jnp.sum(captions * unit_rows(row), axis=1, keepdims=True) + shift
        signs = jnp.where(meta[:, k + 1 : k + 2] > 0.0, 1.0, -1.0)
        value = -signs * logits
        terms = jnp.maximum(value, 0.0) + jnp.log1p(jnp.exp(-jnp.abs(value)))
        loss_ref[k] = jnp.sum(terms * live * used) / total


def finish(first, second, captions, meta, params, gains, weight, total):
    return pl.pallas_call(
        functools.partial(finish_kernel, total),
        out_shape=(
            jax.ShapeDtypeStruct((RECV_MOST, weight.shape[1]), F32),
            jax.ShapeDtypeStruct((RECV_MOST,), F32),
        ),
        in_specs=[smem()] + [vmem()] * 6,
        out_specs=(vmem(), smem()),
        name="finish",
        compiler_params=small(8),
    )(params, gains, weight, captions, meta, first, second)


def per_device(
    pixels,
    selection,
    destination,
    patch_weight,
    position,
    query_key_value,
    output_weight,
    up_weight,
    down_weight,
    norm_gains,
    embedding_weight,
    caption_vectors,
    loss_params,
):
    devices_dp = lax.axis_size("dp")
    shards = lax.axis_size("mp")
    pieces = count_pieces(devices_dp)
    positions, order = gather_blocks(position, "mp")
    rows, caption_meta, piece = pick(
        selection, destination, pixels, caption_vectors, output_weight, pieces
    )
    pixel_blocks = [gather_blocks(row, "mp")[0] for row in rows]

    parts = [swap(piece, "mp", shards // 2)]
    bit = 1
    while bit < pieces:
        parts = parts + [swap(part, "dp", bit) for part in parts]
        bit *= 2
    outputs = [output_weight, assemble(parts)]
    for bit in bits_down(shards)[1:]:
        outputs = outputs + [swap(block, "mp", bit) for block in outputs]

    captions, meta = route(*double_stack(caption_meta, "dp"))

    sums = []
    for r in range(SEND_MOST):
        hidden, context = attend(
            pixel_blocks[r], positions, norm_gains, patch_weight, query_key_value
        )
        contexts, _ = gather_blocks(context, "mp")
        sums.append(expand(contexts, order, outputs, hidden, norm_gains, up_weight))
    pooled = reduce_units(sums, down_weight, position.shape[0] * shards)
    for bit in reversed(bits_down(shards)):
        pooled = add(pooled, swap(pooled, "mp", bit))
    first, second = double_stack(pooled[None], "dp")
    return finish(
        first, second, captions, meta, loss_params, norm_gains, embedding_weight, float(devices_dp * SEL_DEV)
    )


def count_pieces(devices_dp):
    pieces = 1
    while pieces < PIECES and 2 * pieces <= devices_dp:
        pieces *= 2
    return pieces


def solution(mesh):
    in_specs = (
        P("dp", "mp", None),
        P("dp"),
        P("dp"),
        P(),
        P("mp", None),
        P(None, None, "mp"),
        P("mp", None),
        P(None, "mp"),
        P("mp", None),
        P(),
        P(),
        P("dp", None),
        P(),
    )
    out_specs = (P("dp", None), P("dp"))

    return jax.shard_map(
        per_device, mesh=mesh, in_specs=in_specs, out_specs=out_specs, check_vma=False
    )
```

```python
import functools

import jax
import jax.numpy as jnp
from jax import lax
from jax.experimental import pallas as pl
from jax.experimental.pallas import tpu as pltpu
from jax.sharding import PartitionSpec as P


HEAD_DIM = 64
SEL_DEV = 2
SEND_MOST = 3
RECV_MOST = 4
META = 128
PIECES = 2
EPS = 1e-06


VMEM = pltpu.MemorySpace.VMEM
SMEM = pltpu.MemorySpace.SMEM
F32 = jnp.float32
BF16 = jnp.bfloat16


def vmem():
    return pl.BlockSpec(memory_space=VMEM)


def smem():
    return pl.BlockSpec(memory_space=SMEM)


def layer_norm(values, gain):
    center = jnp.mean(values, axis=-1, keepdims=True)
    centred = values - center
    spread = jnp.mean(centred * centred, axis=-1, keepdims=True)
    return centred * lax.rsqrt(spread + EPS) * gain


def unit_rows(values):
    scale = lax.rsqrt(jnp.mean(values * values, axis=-1, keepdims=True) + EPS)
    return values * scale * values.shape[-1] ** (-0.5)


def swap(values, axis, bit):
    size = lax.axis_size(axis)
    return lax.ppermute(values, axis, [(i, i ^ bit) for i in range(size)])


def bits_down(size):
    bits = []
    bit = size // 2
    while bit:
        bits.append(bit)
        bit //= 2
    return bits


def gather_blocks(values, axis):
    blocks, order = [values], [0]
    for bit in bits_down(lax.axis_size(axis)):
        blocks = blocks + [swap(block, axis, bit) for block in blocks]
        order = order + [other ^ bit for other in order]
    return blocks, order


def small(mib):
    return pltpu.CompilerParams(vmem_limit_bytes=mib << 20)


def join_kernel(own_ref, other_ref, out_ref):
    count = own_ref.shape[0]
    out_ref[:count] = own_ref[...]
    out_ref[count:] = other_ref[...]


def join(own, other):
    return pl.pallas_call(
        join_kernel,
        out_shape=jax.ShapeDtypeStruct((2 * own.shape[0],) + own.shape[1:], own.dtype),
        in_specs=[vmem()] * 2,
        out_specs=vmem(),
        compiler_params=small(2),
    )(own, other)


def add_kernel(own_ref, other_ref, out_ref):
    out_ref[...] = own_ref[...] + other_ref[...]


def add(own, other):
    return pl.pallas_call(
        add_kernel,
        out_shape=jax.ShapeDtypeStruct(own.shape, own.dtype),
        in_specs=[vmem()] * 2,
        out_specs=vmem(),
        name="add",
        compiler_params=small(1),
    )(own, other)


def double_stack(values, axis):
    size = lax.axis_size(axis)
    bit = 1
    while 2 * bit < size:
        values = join(values, swap(values, axis, bit))
        bit *= 2
    return values, swap(values, axis, bit)


def pick_kernel(pieces, sel_hbm, dest_hbm, pixels_ref, cap_hbm, output_ref, pos_hbm, *refs):
    row_refs = refs[:SEND_MOST]
    meta_ref, piece_ref, pos_ref, sel_ref, dest_ref, cap_ref, sems = refs[SEND_MOST:]
    first = [
        pltpu.make_async_copy(source, target, sems.at[SEND_MOST + 1 + i])
        for i, (source, target) in enumerate(
            ((sel_hbm, sel_ref), (dest_hbm, dest_ref), (cap_hbm, cap_ref), (pos_hbm, pos_ref))
        )
    ]
    for copy in first:
        copy.start()
    first[0].wait()
    first[1].wait()
    count = jnp.int32(0)
    index = [jnp.int32(0)] * SEND_MOST
    target = [jnp.int32(0)] * SEND_MOST
    for e in range(sel_ref.shape[0]):
        here = sel_ref[e] > 0
        for r in range(SEND_MOST):
            take = here & (count == r)
            index[r] = jnp.where(take, e, index[r])
            target[r] = jnp.where(take, dest_ref[e], target[r])
        count = count + here.astype(jnp.int32)
    copies = [
        pltpu.make_async_copy(pixels_ref.at[index[r]], row_refs[r], sems.at[r])
        for r in range(SEND_MOST)
    ]
    height = piece_ref.shape[0]
    start = pl.multiple_of((lax.axis_index("dp") & (pieces - 1)) * height, height)
    copies.append(
        pltpu.make_async_copy(output_ref.at[pl.ds(start, height)], piece_ref, sems.at[SEND_MOST])
    )
    for copy in copies:
        copy.start()
    first[2].wait()
    captions = cap_ref[...].astype(F32)
    width = captions.shape[1]
    example = lax.broadcasted_iota(jnp.int32, captions.shape, 0)
    lane = lax.broadcasted_iota(jnp.int32, (1, META), 1)
    for r in range(SEND_MOST):
        row = jnp.sum(jnp.where(example == index[r], captions, 0.0), axis=0, keepdims=True)
        live = (count > r).astype(F32)
        extra = jnp.where(lane == 0, live, jnp.where(lane == 1, target[r].astype(F32), 0.0))
        meta_ref[0, r : r + 1, :width] = row.astype(BF16)
        meta_ref[0, r : r + 1, width:] = extra.astype(BF16)
    for copy in copies + first[3:]:
        copy.wait()


def pick(selection, destination, pixels, captions, output_weight, position, pieces):
    _, length, depth = pixels.shape
    fan, width = output_weight.shape
    hbm = pl.BlockSpec(memory_space=pltpu.MemorySpace.HBM)
    *rows, caption_meta, piece, own_position = pl.pallas_call(
        functools.partial(pick_kernel, pieces),
        out_shape=(jax.ShapeDtypeStruct((length, depth), BF16),) * SEND_MOST
        + (
            jax.ShapeDtypeStruct((1, SEND_MOST, captions.shape[1] + META), BF16),
            jax.ShapeDtypeStruct((fan // pieces, width), BF16),
            jax.ShapeDtypeStruct(position.shape, BF16),
        ),
        in_specs=[hbm] * 6,
        out_specs=(vmem(),) * (SEND_MOST + 3),
        scratch_shapes=[
            SMEM(selection.shape, jnp.int32),
            SMEM(destination.shape, jnp.int32),
            VMEM(captions.shape, BF16),
            pltpu.SemaphoreType.DMA((SEND_MOST + 5,)),
        ],
        name="pick",
        compiler_params=small(2),
    )(*(
        pltpu.with_memory_space_constraint(array, pltpu.MemorySpace.HBM)
        for array in (selection, destination, pixels, captions, output_weight, position)
    ))
    return rows, caption_meta, piece, own_position


def load_kernel(source_ref, out_ref, sem):
    copy = pltpu.make_async_copy(source_ref, out_ref, sem)
    copy.start()
    copy.wait()


def load(array):
    return pl.pallas_call(
        load_kernel,
        out_shape=jax.ShapeDtypeStruct(array.shape, array.dtype),
        in_specs=[pl.BlockSpec(memory_space=pltpu.MemorySpace.HBM)],
        out_specs=vmem(),
        scratch_shapes=[pltpu.SemaphoreType.DMA],
        name="load",
        compiler_params=small(2),
    )(pltpu.with_memory_space_constraint(array, pltpu.MemorySpace.HBM))


def assemble_kernel(*refs):
    out_ref = refs[-1]
    pieces = refs[:-1]
    height = pieces[0].shape[0]
    here = lax.axis_index("dp") & (len(pieces) - 1)
    for j, ref in enumerate(pieces):
        start = pl.multiple_of((here ^ j) * height, height)
        out_ref[pl.ds(start, height), :] = ref[...]


def assemble(pieces):
    height, width = pieces[0].shape
    return pl.pallas_call(
        assemble_kernel,
        out_shape=jax.ShapeDtypeStruct((height * len(pieces), width), BF16),
        in_specs=[vmem()] * len(pieces),
        out_specs=vmem(),
        name="assemble",
        compiler_params=small(2),
    )(*pieces)


def route_kernel(first_ref, second_ref, cap_ref, meta_ref):
    half = first_ref.shape[0]
    rows = jnp.concatenate(
        [ref[j].astype(F32) for ref in (first_ref, second_ref) for j in range(half)], axis=0
    )
    width = cap_ref.shape[1]
    cap_ref[...] = unit_rows(rows[:, :width])
    extra = rows[:, width:]
    live, target = extra[:, 0:1], extra[:, 1:2]
    me = lax.axis_index("dp")
    offset = lax.broadcasted_iota(jnp.int32, (SEND_MOST, 1), 0)
    spot = jnp.concatenate([(me ^ j) * SEND_MOST + offset for j in range(2 * half)], axis=0)
    mine = (live > 0.0) & (target == me.astype(F32))
    mine = jnp.where(mine, 1.0, 0.0)
    count = rows.shape[0]
    square = (count, count)
    same = lax.broadcasted_iota(jnp.int32, square, 0) == lax.broadcasted_iota(jnp.int32, square, 1)
    mine_row = jnp.sum(jnp.where(same, mine, 0.0), axis=0, keepdims=True)
    spot_col = spot.astype(F32)
    spot_row = jnp.sum(jnp.where(same, spot_col, 0.0), axis=0, keepdims=True)
    place = jnp.sum(jnp.where(spot_row < spot_col, mine_row, 0.0), axis=1, keepdims=True)
    lane = lax.broadcasted_iota(jnp.int32, (count, META), 1)
    slot = jnp.where(place == (lane - 1).astype(F32), mine, 0.0)
    meta_ref[...] = jnp.where(lane == 0, live, slot)


def route(first, second):
    count = 2 * first.shape[0] * SEND_MOST
    return pl.pallas_call(
        route_kernel,
        out_shape=(
            jax.ShapeDtypeStruct((count, first.shape[2] - META), F32),
            jax.ShapeDtypeStruct((count, META), F32),
        ),
        in_specs=[vmem()] * 2,
        out_specs=(vmem(),) * 2,
        name="route",
        compiler_params=small(6),
    )(first, second)


def attend_kernel(shards, gains_ref, patch_ref, qkv_ref, *refs):
    pixel_refs = refs[:shards]
    position_refs = refs[shards : 2 * shards]
    hidden_ref, context_ref = refs[2 * shards :]
    pixels = jnp.concatenate([ref[...] for ref in pixel_refs], axis=0)
    position = jnp.concatenate([ref[...] for ref in position_refs], axis=0)
    hidden = jnp.dot(pixels, patch_ref[...], preferred_element_type=F32)
    hidden = hidden + position.astype(F32)
    hidden_ref[...] = hidden
    normed = layer_norm(hidden, gains_ref[0:1, :]).astype(BF16)
    query, key, value = [
        jnp.dot(normed, qkv_ref[t], preferred_element_type=F32).astype(BF16) for t in range(3)
    ]
    query = query * jnp.asarray(HEAD_DIM ** (-0.5), BF16)
    parts = []
    for h in range(query.shape[1] // HEAD_DIM):
        cols = slice(h * HEAD_DIM, (h + 1) * HEAD_DIM)
        scores = lax.dot_general(
            query[:, cols], key[:, cols], (((1,), (1,)), ((), ())), preferred_element_type=F32
        )
        weights = jnp.exp(scores - jnp.max(scores, axis=-1, keepdims=True))
        weights = weights * (1.0 / jnp.sum(weights, axis=-1, keepdims=True))
        parts.append(jnp.dot(weights.astype(BF16), value[:, cols], preferred_element_type=F32))
    context_ref[...] = jnp.concatenate(parts, axis=1).astype(BF16)


def attend(pixels, positions, gains, patch_weight, qkv):
    shards = len(pixels)
    length = shards * pixels[0].shape[0]
    width = patch_weight.shape[1]
    return pl.pallas_call(
        functools.partial(attend_kernel, shards),
        out_shape=(
            jax.ShapeDtypeStruct((length, width), F32),
            jax.ShapeDtypeStruct((length, qkv.shape[2]), BF16),
        ),
        in_specs=[vmem()] * (3 + 2 * shards),
        out_specs=(vmem(), vmem()),
        compiler_params=small(14),
    )(gains, patch_weight, qkv, *pixels, *positions)


def expand_kernel(order, gains_ref, up_ref, hidden_ref, *refs):
    shards = len(order)
    context_refs = refs[:shards]
    output_refs = refs[shards : 2 * shards]
    sums_ref = refs[2 * shards]
    block = hidden_ref.shape[0] // shards
    hidden = hidden_ref[...]
    for j, ref in enumerate(context_refs):
        places = [order.index(order[p] ^ order[j]) for p in range(shards)]
        context = jnp.concatenate([ref[q * block : (q + 1) * block, :] for q in places], axis=0)
        hidden = hidden + jnp.dot(context, output_refs[j][...], preferred_element_type=F32)
    normed = layer_norm(hidden, gains_ref[1:2, :]).astype(BF16)
    expanded = jax.nn.gelu(jnp.dot(normed, up_ref[...], preferred_element_type=F32)).astype(BF16)
    sums_ref[0:1, :] = jnp.sum(hidden, axis=0, keepdims=True)
    sums_ref[1:2, :] = jnp.sum(expanded.astype(F32), axis=0, keepdims=True)


def expand(contexts, order, outputs, hidden, gains, up_weight):
    width = hidden.shape[1]
    return pl.pallas_call(
        functools.partial(expand_kernel, tuple(order)),
        out_shape=jax.ShapeDtypeStruct((2, width), F32),
        in_specs=[vmem()] * (3 + 2 * len(order)),
        out_specs=vmem(),
        compiler_params=small(14),
    )(gains, up_weight, hidden, *contexts, *outputs)


def reduce_kernel(scale, down_ref, *refs):
    out_ref = refs[-1]
    sums = refs[:-1]
    units = jnp.concatenate([ref[1:2, :] for ref in sums], axis=0) * scale
    residual = jnp.concatenate([ref[0:1, :] for ref in sums], axis=0) * scale
    high = units.astype(BF16)
    low = (units - high.astype(F32)).astype(BF16)
    both = jnp.concatenate([high, low], axis=0)
    product = jnp.dot(both, down_ref[...], preferred_element_type=F32)
    count = len(sums)
    own = (lax.axis_index("mp") == 0).astype(F32)
    out_ref[...] = product[:count] + product[count:] + residual * own


def reduce_units(sums, down_weight, patches):
    return pl.pallas_call(
        functools.partial(reduce_kernel, 1.0 / patches),
        out_shape=jax.ShapeDtypeStruct((len(sums), down_weight.shape[1]), F32),
        in_specs=[vmem()] * (1 + len(sums)),
        out_specs=vmem(),
        name="reduce",
        compiler_params=small(6),
    )(down_weight, *sums)


def finish_kernel(total, params_ref, gains_ref, weight_ref, cap_ref, meta_ref, first_ref, second_ref, out_ref, loss_ref):
    half = first_ref.shape[0]
    rows = jnp.concatenate(
        [ref[j] for ref in (first_ref, second_ref) for j in range(half)], axis=0
    )
    meta = meta_ref[...]
    live = meta[:, 0:1]
    pooled = jnp.concatenate(
        [
            jnp.sum(jnp.where(meta[:, k + 1 : k + 2] > 0.0, rows, 0.0), axis=0, keepdims=True)
            for k in range(RECV_MOST)
        ],
        axis=0,
    )
    filled = jnp.max(meta, axis=0, keepdims=True)
    normed = layer_norm(pooled, gains_ref[2:3, :]).astype(BF16)
    embedded = jnp.dot(normed, weight_ref[...], preferred_element_type=F32)
    captions = cap_ref[...]
    scale = 10.0 * jnp.exp(jnp.full((1, 1), params_ref[0], F32))
    shift = 2.0 * params_ref[1]
    for k in range(RECV_MOST):
        used = filled[:, k + 1 : k + 2]
        row = jnp.where(used > 0.0, embedded[k : k + 1, :], 0.0)
        out_ref[k : k + 1, :] = row
        logits = scale * jnp.sum(captions * unit_rows(row), axis=1, keepdims=True) + shift
        signs = jnp.where(meta[:, k + 1 : k + 2] > 0.0, 1.0, -1.0)
        value = -signs * logits
        terms = jnp.maximum(value, 0.0) + jnp.log1p(jnp.exp(-jnp.abs(value)))
        loss_ref[k] = jnp.sum(terms * live * used) / total


def finish(first, second, captions, meta, params, gains, weight, total):
    return pl.pallas_call(
        functools.partial(finish_kernel, total),
        out_shape=(
            jax.ShapeDtypeStruct((RECV_MOST, weight.shape[1]), F32),
            jax.ShapeDtypeStruct((RECV_MOST,), F32),
        ),
        in_specs=[smem()] + [vmem()] * 6,
        out_specs=(vmem(), smem()),
        name="finish",
        compiler_params=small(8),
    )(params, gains, weight, captions, meta, first, second)


def per_device(
    pixels,
    selection,
    destination,
    patch_weight,
    position,
    query_key_value,
    output_weight,
    up_weight,
    down_weight,
    norm_gains,
    embedding_weight,
    caption_vectors,
    loss_params,
):
    devices_dp = lax.axis_size("dp")
    shards = lax.axis_size("mp")
    pieces = count_pieces(devices_dp)
    positions, order = gather_blocks(position, "mp")
    rows, caption_meta, piece, own_position = pick(
        selection, destination, pixels, caption_vectors, output_weight, position, pieces
    )
    positions = [own_position] + positions[1:]
    query_key_value = load(query_key_value)
    pixel_blocks = [gather_blocks(row, "mp")[0] for row in rows]

    parts = [swap(piece, "mp", shards // 2)]
    bit = 1
    while bit < pieces:
        parts = parts + [swap(part, "dp", bit) for part in parts]
        bit *= 2
    outputs = [output_weight, assemble(parts)]
    for bit in bits_down(shards)[1:]:
        outputs = outputs + [swap(block, "mp", bit) for block in outputs]

    captions, meta = route(*double_stack(caption_meta, "dp"))

    sums = []
    for r in range(SEND_MOST):
        hidden, context = attend(
            pixel_blocks[r], positions, norm_gains, patch_weight, query_key_value
        )
        contexts, _ = gather_blocks(context, "mp")
        sums.append(expand(contexts, order, outputs, hidden, norm_gains, up_weight))
    pooled = reduce_units(sums, down_weight, position.shape[0] * shards)
    for bit in reversed(bits_down(shards)):
        pooled = add(pooled, swap(pooled, "mp", bit))
    first, second = double_stack(pooled[None], "dp")
    return finish(
        first, second, captions, meta, loss_params, norm_gains, embedding_weight, float(devices_dp * SEL_DEV)
    )


def count_pieces(devices_dp):
    pieces = 1
    while pieces < PIECES and 2 * pieces <= devices_dp:
        pieces *= 2
    return pieces


def solution(mesh):
    in_specs = (
        P("dp", "mp", None),
        P("dp"),
        P("dp"),
        P(),
        P("mp", None),
        P(None, None, "mp"),
        P("mp", None),
        P(None, "mp"),
        P("mp", None),
        P(),
        P(),
        P("dp", None),
        P(),
    )
    out_specs = (P("dp", None), P("dp"))

    return jax.shard_map(
        per_device, mesh=mesh, in_specs=in_specs, out_specs=out_specs, check_vma=False
    )
```

```python
import functools

import jax
import jax.numpy as jnp
from jax import lax
from jax.experimental import pallas as pl
from jax.experimental.pallas import tpu as pltpu
from jax.sharding import PartitionSpec as P


HEAD_DIM = 64
SEL_DEV = 2
SEND_MOST = 3
RECV_MOST = 4
META = 128
PIECES = 2
CHUNKS = (1, 1, 1)
GRANT = 20
EPS = 1e-06


VMEM = pltpu.MemorySpace.VMEM
SMEM = pltpu.MemorySpace.SMEM
F32 = jnp.float32
BF16 = jnp.bfloat16


def vmem():
    return pl.BlockSpec(memory_space=VMEM)


def smem():
    return pl.BlockSpec(memory_space=SMEM)


def layer_norm(values, gain):
    center = jnp.mean(values, axis=-1, keepdims=True)
    centred = values - center
    spread = jnp.mean(centred * centred, axis=-1, keepdims=True)
    return centred * lax.rsqrt(spread + EPS) * gain


def unit_rows(values):
    scale = lax.rsqrt(jnp.mean(values * values, axis=-1, keepdims=True) + EPS)
    return values * scale * values.shape[-1] ** (-0.5)


def swap(values, axis, bit):
    size = lax.axis_size(axis)
    return lax.ppermute(values, axis, [(i, i ^ bit) for i in range(size)])


def bits_down(size):
    bits = []
    bit = size // 2
    while bit:
        bits.append(bit)
        bit //= 2
    return bits


def gather_blocks(values, axis):
    blocks, order = [values], [0]
    for bit in bits_down(lax.axis_size(axis)):
        blocks = blocks + [swap(block, axis, bit) for block in blocks]
        order = order + [other ^ bit for other in order]
    return blocks, order


def small(mib):
    return pltpu.CompilerParams(vmem_limit_bytes=mib << 20)


def join_kernel(own_ref, other_ref, out_ref):
    count = own_ref.shape[0]
    out_ref[:count] = own_ref[...]
    out_ref[count:] = other_ref[...]


def join(own, other):
    return pl.pallas_call(
        join_kernel,
        out_shape=jax.ShapeDtypeStruct((2 * own.shape[0],) + own.shape[1:], own.dtype),
        in_specs=[vmem()] * 2,
        out_specs=vmem(),
        compiler_params=small(2),
    )(own, other)


def add_kernel(own_ref, other_ref, out_ref):
    out_ref[...] = own_ref[...] + other_ref[...]


def add(own, other):
    return pl.pallas_call(
        add_kernel,
        out_shape=jax.ShapeDtypeStruct(own.shape, own.dtype),
        in_specs=[vmem()] * 2,
        out_specs=vmem(),
        name="add",
        compiler_params=small(1),
    )(own, other)


def double_stack(values, axis):
    size = lax.axis_size(axis)
    bit = 1
    while 2 * bit < size:
        values = join(values, swap(values, axis, bit))
        bit *= 2
    return values, swap(values, axis, bit)


def pick_kernel(pieces, sel_hbm, dest_hbm, pixels_ref, cap_hbm, output_ref, pos_hbm, *refs):
    row_refs = refs[: len(CHUNKS)]
    meta_ref, piece_ref, pos_ref, sel_ref, dest_ref, cap_ref, sems = refs[len(CHUNKS) :]
    first = [
        pltpu.make_async_copy(source, target, sems.at[SEND_MOST + 1 + i])
        for i, (source, target) in enumerate(
            ((sel_hbm, sel_ref), (dest_hbm, dest_ref), (cap_hbm, cap_ref), (pos_hbm, pos_ref))
        )
    ]
    for copy in first:
        copy.start()
    first[0].wait()
    first[1].wait()
    count = jnp.int32(0)
    index = [jnp.int32(0)] * SEND_MOST
    target = [jnp.int32(0)] * SEND_MOST
    for e in range(sel_ref.shape[0]):
        here = sel_ref[e] > 0
        for r in range(SEND_MOST):
            take = here & (count == r)
            index[r] = jnp.where(take, e, index[r])
            target[r] = jnp.where(take, dest_ref[e], target[r])
        count = count + here.astype(jnp.int32)
    length = pos_ref.shape[0]
    copies = []
    for c, chunk in enumerate(CHUNKS):
        for i in range(chunk):
            r = sum(CHUNKS[:c]) + i
            place = row_refs[c].at[pl.ds(i * length, length)]
            copies.append(pltpu.make_async_copy(pixels_ref.at[index[r]], place, sems.at[r]))
    height = piece_ref.shape[0]
    start = pl.multiple_of((lax.axis_index("dp") & (pieces - 1)) * height, height)
    copies.append(
        pltpu.make_async_copy(output_ref.at[pl.ds(start, height)], piece_ref, sems.at[SEND_MOST])
    )
    for copy in copies:
        copy.start()
    first[2].wait()
    captions = cap_ref[...].astype(F32)
    width = captions.shape[1]
    example = lax.broadcasted_iota(jnp.int32, captions.shape, 0)
    lane = lax.broadcasted_iota(jnp.int32, (1, META), 1)
    for r in range(SEND_MOST):
        row = jnp.sum(jnp.where(example == index[r], captions, 0.0), axis=0, keepdims=True)
        live = (count > r).astype(F32)
        extra = jnp.where(lane == 0, live, jnp.where(lane == 1, target[r].astype(F32), 0.0))
        meta_ref[0, r : r + 1, :width] = row.astype(BF16)
        meta_ref[0, r : r + 1, width:] = extra.astype(BF16)
    for copy in copies + first[3:]:
        copy.wait()


def pick(selection, destination, pixels, captions, output_weight, position, pieces):
    _, length, depth = pixels.shape
    fan, width = output_weight.shape
    hbm = pl.BlockSpec(memory_space=pltpu.MemorySpace.HBM)
    *rows, caption_meta, piece, own_position = pl.pallas_call(
        functools.partial(pick_kernel, pieces),
        out_shape=tuple(
            jax.ShapeDtypeStruct((chunk * length, depth), BF16) for chunk in CHUNKS
        )
        + (
            jax.ShapeDtypeStruct((1, SEND_MOST, captions.shape[1] + META), BF16),
            jax.ShapeDtypeStruct((fan // pieces, width), BF16),
            jax.ShapeDtypeStruct(position.shape, BF16),
        ),
        in_specs=[hbm] * 6,
        out_specs=(vmem(),) * (len(CHUNKS) + 3),
        scratch_shapes=[
            SMEM(selection.shape, jnp.int32),
            SMEM(destination.shape, jnp.int32),
            VMEM(captions.shape, BF16),
            pltpu.SemaphoreType.DMA((SEND_MOST + 5,)),
        ],
        name="pick",
        compiler_params=small(2),
    )(*(
        pltpu.with_memory_space_constraint(array, pltpu.MemorySpace.HBM)
        for array in (selection, destination, pixels, captions, output_weight, position)
    ))
    return rows, caption_meta, piece, own_position


def load_kernel(source_ref, out_ref, sem):
    copy = pltpu.make_async_copy(source_ref, out_ref, sem)
    copy.start()
    copy.wait()


def load(array):
    return pl.pallas_call(
        load_kernel,
        out_shape=jax.ShapeDtypeStruct(array.shape, array.dtype),
        in_specs=[pl.BlockSpec(memory_space=pltpu.MemorySpace.HBM)],
        out_specs=vmem(),
        scratch_shapes=[pltpu.SemaphoreType.DMA],
        name="load",
        compiler_params=small(2),
    )(pltpu.with_memory_space_constraint(array, pltpu.MemorySpace.HBM))


def assemble_kernel(*refs):
    out_ref = refs[-1]
    pieces = refs[:-1]
    height = pieces[0].shape[0]
    here = lax.axis_index("dp") & (len(pieces) - 1)
    for j, ref in enumerate(pieces):
        start = pl.multiple_of((here ^ j) * height, height)
        out_ref[pl.ds(start, height), :] = ref[...]


def assemble(pieces):
    height, width = pieces[0].shape
    return pl.pallas_call(
        assemble_kernel,
        out_shape=jax.ShapeDtypeStruct((height * len(pieces), width), BF16),
        in_specs=[vmem()] * len(pieces),
        out_specs=vmem(),
        name="assemble",
        compiler_params=small(2),
    )(*pieces)


def route_kernel(first_ref, second_ref, cap_ref, meta_ref):
    half = first_ref.shape[0]
    rows = jnp.concatenate(
        [ref[j].astype(F32) for ref in (first_ref, second_ref) for j in range(half)], axis=0
    )
    width = cap_ref.shape[1]
    cap_ref[...] = unit_rows(rows[:, :width])
    extra = rows[:, width:]
    live, target = extra[:, 0:1], extra[:, 1:2]
    me = lax.axis_index("dp")
    offset = lax.broadcasted_iota(jnp.int32, (SEND_MOST, 1), 0)
    spot = jnp.concatenate([(me ^ j) * SEND_MOST + offset for j in range(2 * half)], axis=0)
    mine = (live > 0.0) & (target == me.astype(F32))
    mine = jnp.where(mine, 1.0, 0.0)
    count = rows.shape[0]
    square = (count, count)
    same = lax.broadcasted_iota(jnp.int32, square, 0) == lax.broadcasted_iota(jnp.int32, square, 1)
    mine_row = jnp.sum(jnp.where(same, mine, 0.0), axis=0, keepdims=True)
    spot_col = spot.astype(F32)
    spot_row = jnp.sum(jnp.where(same, spot_col, 0.0), axis=0, keepdims=True)
    place = jnp.sum(jnp.where(spot_row < spot_col, mine_row, 0.0), axis=1, keepdims=True)
    lane = lax.broadcasted_iota(jnp.int32, (count, META), 1)
    slot = jnp.where(place == (lane - 1).astype(F32), mine, 0.0)
    meta_ref[...] = jnp.where(lane == 0, live, slot)


def route(first, second):
    count = 2 * first.shape[0] * SEND_MOST
    return pl.pallas_call(
        route_kernel,
        out_shape=(
            jax.ShapeDtypeStruct((count, first.shape[2] - META), F32),
            jax.ShapeDtypeStruct((count, META), F32),
        ),
        in_specs=[vmem()] * 2,
        out_specs=(vmem(),) * 2,
        name="route",
        compiler_params=small(6),
    )(first, second)


def attend_kernel(shards, gains_ref, patch_ref, qkv_ref, *refs):
    pixel_refs = refs[:shards]
    position_refs = refs[shards : 2 * shards]
    hidden_ref, context_ref = refs[2 * shards :]
    block = position_refs[0].shape[0]
    length = block * shards
    images = range(pixel_refs[0].shape[0] // block)
    pixels = jnp.concatenate(
        [ref[i * block : (i + 1) * block, :] for i in images for ref in pixel_refs], axis=0
    )
    position = jnp.concatenate([ref[...] for ref in position_refs], axis=0).astype(F32)
    hidden = jnp.dot(pixels, patch_ref[...], preferred_element_type=F32)
    hidden = hidden + jnp.concatenate([position for _ in images], axis=0)
    hidden_ref[...] = hidden
    normed = layer_norm(hidden, gains_ref[0:1, :]).astype(BF16)
    query, key, value = [
        jnp.dot(normed, qkv_ref[t], preferred_element_type=F32).astype(BF16) for t in range(3)
    ]
    query = query * jnp.asarray(HEAD_DIM ** (-0.5), BF16)
    for i in images:
        rows = slice(i * length, (i + 1) * length)
        parts = []
        for h in range(query.shape[1] // HEAD_DIM):
            cols = slice(h * HEAD_DIM, (h + 1) * HEAD_DIM)
            scores = lax.dot_general(
                query[rows, cols],
                key[rows, cols],
                (((1,), (1,)), ((), ())),
                preferred_element_type=F32,
            )
            weights = jnp.exp(scores - jnp.max(scores, axis=-1, keepdims=True))
            weights = weights * (1.0 / jnp.sum(weights, axis=-1, keepdims=True))
            parts.append(
                jnp.dot(weights.astype(BF16), value[rows, cols], preferred_element_type=F32)
            )
        context_ref[rows, :] = jnp.concatenate(parts, axis=1).astype(BF16)


def attend(pixels, positions, gains, patch_weight, qkv):
    shards = len(pixels)
    length = shards * pixels[0].shape[0]
    width = patch_weight.shape[1]
    return pl.pallas_call(
        functools.partial(attend_kernel, shards),
        out_shape=(
            jax.ShapeDtypeStruct((length, width), F32),
            jax.ShapeDtypeStruct((length, qkv.shape[2]), BF16),
        ),
        in_specs=[vmem()] * (3 + 2 * shards),
        out_specs=(vmem(), vmem()),
        compiler_params=small(GRANT),
    )(gains, patch_weight, qkv, *pixels, *positions)


def expand_kernel(order, images, gains_ref, up_ref, hidden_ref, *refs):
    shards = len(order)
    context_refs = refs[:shards]
    output_refs = refs[shards : 2 * shards]
    sums_ref = refs[2 * shards]
    length = hidden_ref.shape[0] // images
    block = length // shards
    hidden = hidden_ref[...]
    for j, ref in enumerate(context_refs):
        places = [order.index(order[p] ^ order[j]) for p in range(shards)]
        starts = [i * length + q * block for i in range(images) for q in places]
        context = jnp.concatenate([ref[at : at + block, :] for at in starts], axis=0)
        hidden = hidden + jnp.dot(context, output_refs[j][...], preferred_element_type=F32)
    normed = layer_norm(hidden, gains_ref[1:2, :]).astype(BF16)
    expanded = jax.nn.gelu(jnp.dot(normed, up_ref[...], preferred_element_type=F32)).astype(BF16)
    expanded = expanded.astype(F32)
    for i in range(images):
        rows = slice(i * length, (i + 1) * length)
        sums_ref[i : i + 1, :] = jnp.sum(hidden[rows], axis=0, keepdims=True)
        sums_ref[images + i : images + i + 1, :] = jnp.sum(expanded[rows], axis=0, keepdims=True)


def expand(contexts, order, images, outputs, hidden, gains, up_weight):
    width = hidden.shape[1]
    return pl.pallas_call(
        functools.partial(expand_kernel, tuple(order), images),
        out_shape=jax.ShapeDtypeStruct((2 * images, width), F32),
        in_specs=[vmem()] * (3 + 2 * len(order)),
        out_specs=vmem(),
        compiler_params=small(GRANT),
    )(gains, up_weight, hidden, *contexts, *outputs)


def reduce_kernel(scale, down_ref, *refs):
    out_ref = refs[-1]
    sums = refs[:-1]
    halves = [ref.shape[0] // 2 for ref in sums]
    units = jnp.concatenate([ref[n:, :] for n, ref in zip(halves, sums)], axis=0) * scale
    residual = jnp.concatenate([ref[:n, :] for n, ref in zip(halves, sums)], axis=0) * scale
    high = units.astype(BF16)
    low = (units - high.astype(F32)).astype(BF16)
    both = jnp.concatenate([high, low], axis=0)
    product = jnp.dot(both, down_ref[...], preferred_element_type=F32)
    count = sum(halves)
    own = (lax.axis_index("mp") == 0).astype(F32)
    out_ref[...] = product[:count] + product[count:] + residual * own


def reduce_units(sums, down_weight, patches):
    return pl.pallas_call(
        functools.partial(reduce_kernel, 1.0 / patches),
        out_shape=jax.ShapeDtypeStruct((SEND_MOST, down_weight.shape[1]), F32),
        in_specs=[vmem()] * (1 + len(sums)),
        out_specs=vmem(),
        name="reduce",
        compiler_params=small(6),
    )(down_weight, *sums)


def finish_kernel(total, params_ref, gains_ref, weight_ref, cap_ref, meta_ref, first_ref, second_ref, out_ref, loss_ref):
    half = first_ref.shape[0]
    rows = jnp.concatenate(
        [ref[j] for ref in (first_ref, second_ref) for j in range(half)], axis=0
    )
    meta = meta_ref[...]
    live = meta[:, 0:1]
    pooled = jnp.concatenate(
        [
            jnp.sum(jnp.where(meta[:, k + 1 : k + 2] > 0.0, rows, 0.0), axis=0, keepdims=True)
            for k in range(RECV_MOST)
        ],
        axis=0,
    )
    filled = jnp.max(meta, axis=0, keepdims=True)
    normed = layer_norm(pooled, gains_ref[2:3, :]).astype(BF16)
    embedded = jnp.dot(normed, weight_ref[...], preferred_element_type=F32)
    captions = cap_ref[...]
    scale = 10.0 * jnp.exp(jnp.full((1, 1), params_ref[0], F32))
    shift = 2.0 * params_ref[1]
    for k in range(RECV_MOST):
        used = filled[:, k + 1 : k + 2]
        row = jnp.where(used > 0.0, embedded[k : k + 1, :], 0.0)
        out_ref[k : k + 1, :] = row
        logits = scale * jnp.sum(captions * unit_rows(row), axis=1, keepdims=True) + shift
        signs = jnp.where(meta[:, k + 1 : k + 2] > 0.0, 1.0, -1.0)
        value = -signs * logits
        terms = jnp.maximum(value, 0.0) + jnp.log1p(jnp.exp(-jnp.abs(value)))
        loss_ref[k] = jnp.sum(terms * live * used) / total


def finish(first, second, captions, meta, params, gains, weight, total):
    return pl.pallas_call(
        functools.partial(finish_kernel, total),
        out_shape=(
            jax.ShapeDtypeStruct((RECV_MOST, weight.shape[1]), F32),
            jax.ShapeDtypeStruct((RECV_MOST,), F32),
        ),
        in_specs=[smem()] + [vmem()] * 6,
        out_specs=(vmem(), smem()),
        name="finish",
        compiler_params=small(8),
    )(params, gains, weight, captions, meta, first, second)


def per_device(
    pixels,
    selection,
    destination,
    patch_weight,
    position,
    query_key_value,
    output_weight,
    up_weight,
    down_weight,
    norm_gains,
    embedding_weight,
    caption_vectors,
    loss_params,
):
    devices_dp = lax.axis_size("dp")
    shards = lax.axis_size("mp")
    pieces = count_pieces(devices_dp)
    positions, order = gather_blocks(position, "mp")
    rows, caption_meta, piece, own_position = pick(
        selection, destination, pixels, caption_vectors, output_weight, position, pieces
    )
    positions = [own_position] + positions[1:]
    query_key_value = load(query_key_value)
    pixel_blocks = [gather_blocks(row, "mp")[0] for row in rows]

    parts = [swap(piece, "mp", shards // 2)]
    bit = 1
    while bit < pieces:
        parts = parts + [swap(part, "dp", bit) for part in parts]
        bit *= 2
    outputs = [output_weight, assemble(parts)]
    for bit in bits_down(shards)[1:]:
        outputs = outputs + [swap(block, "mp", bit) for block in outputs]

    captions, meta = route(*double_stack(caption_meta, "dp"))

    sums = []
    for r, images in enumerate(CHUNKS):
        hidden, context = attend(
            pixel_blocks[r], positions, norm_gains, patch_weight, query_key_value
        )
        contexts, _ = gather_blocks(context, "mp")
        sums.append(expand(contexts, order, images, outputs, hidden, norm_gains, up_weight))
    pooled = reduce_units(sums, down_weight, position.shape[0] * shards)
    for bit in reversed(bits_down(shards)):
        pooled = add(pooled, swap(pooled, "mp", bit))
    first, second = double_stack(pooled[None], "dp")
    return finish(
        first, second, captions, meta, loss_params, norm_gains, embedding_weight, float(devices_dp * SEL_DEV)
    )


def count_pieces(devices_dp):
    pieces = 1
    while pieces < PIECES and 2 * pieces <= devices_dp:
        pieces *= 2
    return pieces


def solution(mesh):
    in_specs = (
        P("dp", "mp", None),
        P("dp"),
        P("dp"),
        P(),
        P("mp", None),
        P(None, None, "mp"),
        P("mp", None),
        P(None, "mp"),
        P("mp", None),
        P(),
        P(),
        P("dp", None),
        P(),
    )
    out_specs = (P("dp", None), P("dp"))

    return jax.shard_map(
        per_device, mesh=mesh, in_specs=in_specs, out_specs=out_specs, check_vma=False
    )
```

```python
import functools

import jax
import jax.numpy as jnp
from jax import lax
from jax.experimental import pallas as pl
from jax.experimental.pallas import tpu as pltpu
from jax.sharding import PartitionSpec as P


HEAD_DIM = 64
SEL_DEV = 2
SEND_MOST = 3
RECV_MOST = 4
META = 128
PIECES = 2
CHUNKS = (1, 1, 1)
GRANT = 20
EPS = 1e-06


VMEM = pltpu.MemorySpace.VMEM
SMEM = pltpu.MemorySpace.SMEM
F32 = jnp.float32
BF16 = jnp.bfloat16


def vmem():
    return pl.BlockSpec(memory_space=VMEM)


def smem():
    return pl.BlockSpec(memory_space=SMEM)


def layer_norm(values, gain):
    center = jnp.mean(values, axis=-1, keepdims=True)
    centred = values - center
    spread = jnp.mean(centred * centred, axis=-1, keepdims=True)
    return centred * lax.rsqrt(spread + EPS) * gain


def unit_rows(values):
    scale = lax.rsqrt(jnp.mean(values * values, axis=-1, keepdims=True) + EPS)
    return values * scale * values.shape[-1] ** (-0.5)


def swap(values, axis, bit):
    size = lax.axis_size(axis)
    return lax.ppermute(values, axis, [(i, i ^ bit) for i in range(size)])


def bits_down(size):
    bits = []
    bit = size // 2
    while bit:
        bits.append(bit)
        bit //= 2
    return bits


def gather_blocks(values, axis):
    blocks, order = [values], [0]
    for bit in bits_down(lax.axis_size(axis)):
        blocks = blocks + [swap(block, axis, bit) for block in blocks]
        order = order + [other ^ bit for other in order]
    return blocks, order


def small(mib):
    return pltpu.CompilerParams(vmem_limit_bytes=mib << 20)


def join_kernel(own_ref, other_ref, out_ref):
    count = own_ref.shape[0]
    out_ref[:count] = own_ref[...]
    out_ref[count:] = other_ref[...]


def join(own, other):
    return pl.pallas_call(
        join_kernel,
        out_shape=jax.ShapeDtypeStruct((2 * own.shape[0],) + own.shape[1:], own.dtype),
        in_specs=[vmem()] * 2,
        out_specs=vmem(),
        compiler_params=small(2),
    )(own, other)


def add_kernel(own_ref, other_ref, out_ref):
    out_ref[...] = own_ref[...] + other_ref[...]


def add(own, other):
    return pl.pallas_call(
        add_kernel,
        out_shape=jax.ShapeDtypeStruct(own.shape, own.dtype),
        in_specs=[vmem()] * 2,
        out_specs=vmem(),
        name="add",
        compiler_params=small(1),
    )(own, other)


def double_stack(values, axis):
    size = lax.axis_size(axis)
    bit = 1
    while 2 * bit < size:
        values = join(values, swap(values, axis, bit))
        bit *= 2
    return values, swap(values, axis, bit)


def pick_kernel(pieces, sel_hbm, dest_hbm, pixels_ref, cap_hbm, output_ref, pos_hbm, *refs):
    row_refs = refs[: len(CHUNKS)]
    meta_ref, piece_ref, pos_ref, sel_ref, dest_ref, cap_ref, sems = refs[len(CHUNKS) :]
    first = [
        pltpu.make_async_copy(source, target, sems.at[SEND_MOST + 1 + i])
        for i, (source, target) in enumerate(
            ((sel_hbm, sel_ref), (dest_hbm, dest_ref), (cap_hbm, cap_ref), (pos_hbm, pos_ref))
        )
    ]
    for copy in first:
        copy.start()
    first[0].wait()
    first[1].wait()
    count = jnp.int32(0)
    index = [jnp.int32(0)] * SEND_MOST
    target = [jnp.int32(0)] * SEND_MOST
    for e in range(sel_ref.shape[0]):
        here = sel_ref[e] > 0
        for r in range(SEND_MOST):
            take = here & (count == r)
            index[r] = jnp.where(take, e, index[r])
            target[r] = jnp.where(take, dest_ref[e], target[r])
        count = count + here.astype(jnp.int32)
    length = pos_ref.shape[0]
    copies = []
    for c, chunk in enumerate(CHUNKS):
        for i in range(chunk):
            r = sum(CHUNKS[:c]) + i
            place = row_refs[c].at[pl.ds(i * length, length)]
            copies.append(pltpu.make_async_copy(pixels_ref.at[index[r]], place, sems.at[r]))
    height = piece_ref.shape[0]
    start = pl.multiple_of((lax.axis_index("dp") & (pieces - 1)) * height, height)
    copies.append(
        pltpu.make_async_copy(output_ref.at[pl.ds(start, height)], piece_ref, sems.at[SEND_MOST])
    )
    for copy in copies:
        copy.start()
    first[2].wait()
    captions = cap_ref[...].astype(F32)
    width = captions.shape[1]
    example = lax.broadcasted_iota(jnp.int32, captions.shape, 0)
    lane = lax.broadcasted_iota(jnp.int32, (1, META), 1)
    for r in range(SEND_MOST):
        row = jnp.sum(jnp.where(example == index[r], captions, 0.0), axis=0, keepdims=True)
        live = (count > r).astype(F32)
        extra = jnp.where(lane == 0, live, jnp.where(lane == 1, target[r].astype(F32), 0.0))
        meta_ref[0, r : r + 1, :width] = row.astype(BF16)
        meta_ref[0, r : r + 1, width:] = extra.astype(BF16)
    for copy in copies + first[3:]:
        copy.wait()


def pick(selection, destination, pixels, captions, output_weight, position, pieces):
    _, length, depth = pixels.shape
    fan, width = output_weight.shape
    hbm = pl.BlockSpec(memory_space=pltpu.MemorySpace.HBM)
    *rows, caption_meta, piece, own_position = pl.pallas_call(
        functools.partial(pick_kernel, pieces),
        out_shape=tuple(
            jax.ShapeDtypeStruct((chunk * length, depth), BF16) for chunk in CHUNKS
        )
        + (
            jax.ShapeDtypeStruct((1, SEND_MOST, captions.shape[1] + META), BF16),
            jax.ShapeDtypeStruct((fan // pieces, width), BF16),
            jax.ShapeDtypeStruct(position.shape, BF16),
        ),
        in_specs=[hbm] * 6,
        out_specs=(vmem(),) * (len(CHUNKS) + 3),
        scratch_shapes=[
            SMEM(selection.shape, jnp.int32),
            SMEM(destination.shape, jnp.int32),
            VMEM(captions.shape, BF16),
            pltpu.SemaphoreType.DMA((SEND_MOST + 5,)),
        ],
        name="pick",
        compiler_params=small(2),
    )(*(
        pltpu.with_memory_space_constraint(array, pltpu.MemorySpace.HBM)
        for array in (selection, destination, pixels, captions, output_weight, position)
    ))
    return rows, caption_meta, piece, own_position


def load_kernel(source_ref, out_ref, sem):
    copy = pltpu.make_async_copy(source_ref, out_ref, sem)
    copy.start()
    copy.wait()


def load(array):
    return pl.pallas_call(
        load_kernel,
        out_shape=jax.ShapeDtypeStruct(array.shape, array.dtype),
        in_specs=[pl.BlockSpec(memory_space=pltpu.MemorySpace.HBM)],
        out_specs=vmem(),
        scratch_shapes=[pltpu.SemaphoreType.DMA],
        name="load",
        compiler_params=small(2),
    )(pltpu.with_memory_space_constraint(array, pltpu.MemorySpace.HBM))


def assemble_kernel(*refs):
    out_ref = refs[-1]
    pieces = refs[:-1]
    height = pieces[0].shape[0]
    here = lax.axis_index("dp") & (len(pieces) - 1)
    for j, ref in enumerate(pieces):
        start = pl.multiple_of((here ^ j) * height, height)
        out_ref[pl.ds(start, height), :] = ref[...]


def assemble(pieces):
    height, width = pieces[0].shape
    return pl.pallas_call(
        assemble_kernel,
        out_shape=jax.ShapeDtypeStruct((height * len(pieces), width), BF16),
        in_specs=[vmem()] * len(pieces),
        out_specs=vmem(),
        name="assemble",
        compiler_params=small(2),
    )(*pieces)


def route_kernel(params_ref, first_ref, second_ref, cap_ref, slot_ref, live_ref, line_ref):
    half = first_ref.shape[0]
    rows = jnp.concatenate(
        [ref[j].astype(F32) for ref in (first_ref, second_ref) for j in range(half)], axis=0
    )
    width = cap_ref.shape[1]
    cap_ref[...] = unit_rows(rows[:, :width])
    extra = rows[:, width:]
    live, target = extra[:, 0:1], extra[:, 1:2]
    me = lax.axis_index("dp")
    offset = lax.broadcasted_iota(jnp.int32, (SEND_MOST, 1), 0)
    spot = jnp.concatenate([(me ^ j) * SEND_MOST + offset for j in range(2 * half)], axis=0)
    mine = (live > 0.0) & (target == me.astype(F32))
    mine = jnp.where(mine, 1.0, 0.0)
    count = rows.shape[0]
    square = (count, count)
    same = lax.broadcasted_iota(jnp.int32, square, 0) == lax.broadcasted_iota(jnp.int32, square, 1)
    mine_row = jnp.sum(jnp.where(same, mine, 0.0), axis=0, keepdims=True)
    spot_col = spot.astype(F32)
    spot_row = jnp.sum(jnp.where(same, spot_col, 0.0), axis=0, keepdims=True)
    place = jnp.sum(jnp.where(spot_row < spot_col, mine_row, 0.0), axis=1, keepdims=True)
    lane = lax.broadcasted_iota(jnp.int32, (count, META), 1)
    slot_ref[...] = jnp.where(place == lane.astype(F32), mine, 0.0)
    live_ref[...] = jnp.broadcast_to(live, (count, META))
    row = lax.broadcasted_iota(jnp.int32, line_ref.shape, 0)
    scale = 10.0 * jnp.exp(jnp.full(line_ref.shape, params_ref[0], F32))
    line_ref[...] = jnp.where(row == 0, scale, 2.0 * params_ref[1])


def route(first, second, params):
    count = 2 * first.shape[0] * SEND_MOST
    return pl.pallas_call(
        route_kernel,
        out_shape=(
            jax.ShapeDtypeStruct((count, first.shape[2] - META), F32),
            jax.ShapeDtypeStruct((count, META), F32),
            jax.ShapeDtypeStruct((count, META), F32),
            jax.ShapeDtypeStruct((2, META), F32),
        ),
        in_specs=[smem()] + [vmem()] * 2,
        out_specs=(vmem(),) * 4,
        name="route",
        compiler_params=small(6),
    )(params, first, second)


def attend_kernel(shards, gains_ref, patch_ref, qkv_ref, *refs):
    pixel_refs = refs[:shards]
    position_refs = refs[shards : 2 * shards]
    hidden_ref, context_ref = refs[2 * shards :]
    block = position_refs[0].shape[0]
    length = block * shards
    images = range(pixel_refs[0].shape[0] // block)
    pixels = jnp.concatenate(
        [ref[i * block : (i + 1) * block, :] for i in images for ref in pixel_refs], axis=0
    )
    position = jnp.concatenate([ref[...] for ref in position_refs], axis=0).astype(F32)
    hidden = jnp.dot(pixels, patch_ref[...], preferred_element_type=F32)
    hidden = hidden + jnp.concatenate([position for _ in images], axis=0)
    hidden_ref[...] = hidden
    normed = layer_norm(hidden, gains_ref[0:1, :]).astype(BF16)
    query, key, value = [
        jnp.dot(normed, qkv_ref[t], preferred_element_type=F32).astype(BF16) for t in range(3)
    ]
    query = query * jnp.asarray(HEAD_DIM ** (-0.5), BF16)
    for i in images:
        rows = slice(i * length, (i + 1) * length)
        parts = []
        for h in range(query.shape[1] // HEAD_DIM):
            cols = slice(h * HEAD_DIM, (h + 1) * HEAD_DIM)
            scores = lax.dot_general(
                query[rows, cols],
                key[rows, cols],
                (((1,), (1,)), ((), ())),
                preferred_element_type=F32,
            )
            weights = jnp.exp(scores - jnp.max(scores, axis=-1, keepdims=True))
            weights = weights * (1.0 / jnp.sum(weights, axis=-1, keepdims=True))
            parts.append(
                jnp.dot(weights.astype(BF16), value[rows, cols], preferred_element_type=F32)
            )
        context_ref[rows, :] = jnp.concatenate(parts, axis=1).astype(BF16)


def attend(pixels, positions, gains, patch_weight, qkv):
    shards = len(pixels)
    length = shards * pixels[0].shape[0]
    width = patch_weight.shape[1]
    return pl.pallas_call(
        functools.partial(attend_kernel, shards),
        out_shape=(
            jax.ShapeDtypeStruct((length, width), F32),
            jax.ShapeDtypeStruct((length, qkv.shape[2]), BF16),
        ),
        in_specs=[vmem()] * (3 + 2 * shards),
        out_specs=(vmem(), vmem()),
        compiler_params=small(GRANT),
    )(gains, patch_weight, qkv, *pixels, *positions)


def mix(hidden, order, which, images, context_refs, output_refs):
    shards = len(order)
    length = hidden.shape[0] // images
    block = length // shards
    for j, context_ref, output_ref in zip(which, context_refs, output_refs):
        places = [order.index(order[p] ^ order[j]) for p in range(shards)]
        starts = [i * length + q * block for i in range(images) for q in places]
        context = jnp.concatenate([context_ref[at : at + block, :] for at in starts], axis=0)
        hidden = hidden + jnp.dot(context, output_ref[...], preferred_element_type=F32)
    return hidden


def blend_kernel(order, which, images, hidden_ref, *refs):
    count = len(which)
    hidden = hidden_ref[...]
    refs[-1][...] = mix(hidden, order, which, images, refs[:count], refs[count : 2 * count])


def blend(contexts, order, which, images, outputs, hidden):
    return pl.pallas_call(
        functools.partial(blend_kernel, tuple(order), tuple(which), images),
        out_shape=jax.ShapeDtypeStruct(hidden.shape, F32),
        in_specs=[vmem()] * (1 + 2 * len(which)),
        out_specs=vmem(),
        compiler_params=small(GRANT),
    )(hidden, *(contexts[j] for j in which), *(outputs[j] for j in which))


def expand_kernel(order, which, images, gains_ref, up_ref, hidden_ref, *refs):
    count = len(which)
    sums_ref = refs[2 * count]
    length = hidden_ref.shape[0] // images
    hidden = mix(hidden_ref[...], order, which, images, refs[:count], refs[count : 2 * count])
    normed = layer_norm(hidden, gains_ref[1:2, :]).astype(BF16)
    expanded = jax.nn.gelu(jnp.dot(normed, up_ref[...], preferred_element_type=F32)).astype(BF16)
    expanded = expanded.astype(F32)
    for i in range(images):
        rows = slice(i * length, (i + 1) * length)
        sums_ref[i : i + 1, :] = jnp.sum(hidden[rows], axis=0, keepdims=True)
        sums_ref[images + i : images + i + 1, :] = jnp.sum(expanded[rows], axis=0, keepdims=True)


def expand(contexts, order, which, images, outputs, hidden, gains, up_weight):
    width = hidden.shape[1]
    return pl.pallas_call(
        functools.partial(expand_kernel, tuple(order), tuple(which), images),
        out_shape=jax.ShapeDtypeStruct((2 * images, width), F32),
        in_specs=[vmem()] * (3 + 2 * len(which)),
        out_specs=vmem(),
        compiler_params=small(GRANT),
    )(gains, up_weight, hidden, *(contexts[j] for j in which), *(outputs[j] for j in which))


def reduce_kernel(scale, down_ref, *refs):
    out_ref = refs[-1]
    sums = refs[:-1]
    halves = [ref.shape[0] // 2 for ref in sums]
    units = jnp.concatenate([ref[n:, :] for n, ref in zip(halves, sums)], axis=0) * scale
    residual = jnp.concatenate([ref[:n, :] for n, ref in zip(halves, sums)], axis=0) * scale
    high = units.astype(BF16)
    low = (units - high.astype(F32)).astype(BF16)
    both = jnp.concatenate([high, low], axis=0)
    product = jnp.dot(both, down_ref[...], preferred_element_type=F32)
    count = sum(halves)
    own = (lax.axis_index("mp") == 0).astype(F32)
    out_ref[...] = product[:count] + product[count:] + residual * own


def reduce_units(sums, down_weight, patches):
    return pl.pallas_call(
        functools.partial(reduce_kernel, 1.0 / patches),
        out_shape=jax.ShapeDtypeStruct((SEND_MOST, down_weight.shape[1]), F32),
        in_specs=[vmem()] * (1 + len(sums)),
        out_specs=vmem(),
        name="reduce",
        compiler_params=small(6),
    )(down_weight, *sums)


def finish_kernel(total, gains_ref, weight_ref, cap_ref, slot_ref, live_ref, line_ref, *refs):
    first_ref, second_ref, out_ref, loss_ref = refs
    half = first_ref.shape[0]
    rows = jnp.concatenate(
        [ref[j] for ref in (first_ref, second_ref) for j in range(half)], axis=0
    )
    slot = slot_ref[...]
    pooled = jnp.concatenate(
        [
            jnp.sum(jnp.where(slot[:, k : k + 1] > 0.0, rows, 0.0), axis=0, keepdims=True)
            for k in range(RECV_MOST)
        ],
        axis=0,
    )
    filled = jnp.max(slot, axis=0, keepdims=True)
    used = jnp.concatenate([filled[:, k : k + 1] for k in range(RECV_MOST)], axis=0)
    normed = layer_norm(pooled, gains_ref[2:3, :]).astype(BF16)
    embedded = jnp.dot(normed, weight_ref[...], preferred_element_type=F32)
    embedded = jnp.where(used > 0.0, embedded, 0.0)
    out_ref[...] = embedded
    captions = cap_ref[...]
    images = unit_rows(embedded)
    lane = lax.broadcasted_iota(jnp.int32, slot.shape, 1)
    products = jnp.zeros(slot.shape, F32)
    for k in range(RECV_MOST):
        product = jnp.sum(captions * images[k : k + 1, :], axis=1, keepdims=True)
        products = jnp.where(lane == k, product, products)
    logits = line_ref[0:1, :] * products + line_ref[1:2, :]
    value = jnp.where(slot > 0.0, -logits, logits)
    terms = jnp.maximum(value, 0.0) + jnp.log1p(jnp.exp(-jnp.abs(value)))
    losses = jnp.sum(terms * live_ref[...], axis=0, keepdims=True) * (1.0 / total) * filled
    loss_ref[...] = losses[0, :RECV_MOST]


def finish(first, second, routed, gains, weight, total):
    return pl.pallas_call(
        functools.partial(finish_kernel, total),
        out_shape=(
            jax.ShapeDtypeStruct((RECV_MOST, weight.shape[1]), F32),
            jax.ShapeDtypeStruct((RECV_MOST,), F32),
        ),
        in_specs=[vmem()] * 8,
        out_specs=(vmem(), vmem()),
        name="finish",
        compiler_params=small(8),
    )(gains, weight, *routed, first, second)


def per_device(
    pixels,
    selection,
    destination,
    patch_weight,
    position,
    query_key_value,
    output_weight,
    up_weight,
    down_weight,
    norm_gains,
    embedding_weight,
    caption_vectors,
    loss_params,
):
    devices_dp = lax.axis_size("dp")
    shards = lax.axis_size("mp")
    pieces = count_pieces(devices_dp)
    positions, order = gather_blocks(position, "mp")
    rows, caption_meta, piece, own_position = pick(
        selection, destination, pixels, caption_vectors, output_weight, position, pieces
    )
    positions = [own_position] + positions[1:]
    query_key_value = load(query_key_value)
    pixel_blocks = [gather_blocks(row, "mp")[0] for row in rows]

    parts = [swap(piece, "mp", shards // 2)]
    bit = 1
    while bit < pieces:
        parts = parts + [swap(part, "dp", bit) for part in parts]
        bit *= 2
    outputs = [output_weight, assemble(parts)]
    for bit in bits_down(shards)[1:]:
        outputs = outputs + [swap(block, "mp", bit) for block in outputs]

    routed = route(*double_stack(caption_meta, "dp"), loss_params)

    sums = []
    for r, images in enumerate(CHUNKS):
        hidden, context = attend(
            pixel_blocks[r], positions, norm_gains, patch_weight, query_key_value
        )
        contexts, _ = gather_blocks(context, "mp")
        which = list(range(shards))
        if r == len(CHUNKS) - 1:
            hidden = blend(contexts, order, which[:-1], images, outputs, hidden)
            which = which[-1:]
        sums.append(expand(contexts, order, which, images, outputs, hidden, norm_gains, up_weight))
    pooled = reduce_units(sums, down_weight, position.shape[0] * shards)
    for bit in reversed(bits_down(shards)):
        pooled = add(pooled, swap(pooled, "mp", bit))
    first, second = double_stack(pooled[None], "dp")
    return finish(
        first, second, routed, norm_gains, embedding_weight, float(devices_dp * SEL_DEV)
    )


def count_pieces(devices_dp):
    pieces = 1
    while pieces < PIECES and 2 * pieces <= devices_dp:
        pieces *= 2
    return pieces


def solution(mesh):
    in_specs = (
        P("dp", "mp", None),
        P("dp"),
        P("dp"),
        P(),
        P("mp", None),
        P(None, None, "mp"),
        P("mp", None),
        P(None, "mp"),
        P("mp", None),
        P(),
        P(),
        P("dp", None),
        P(),
    )
    out_specs = (P("dp", None), P("dp"))

    return jax.shard_map(
        per_device, mesh=mesh, in_specs=in_specs, out_specs=out_specs, check_vma=False
    )
```

```python
import functools

import jax
import jax.numpy as jnp
from jax import lax
from jax.experimental import pallas as pl
from jax.experimental.pallas import tpu as pltpu
from jax.sharding import PartitionSpec as P


HEAD_DIM = 64
SEL_DEV = 2
SEND_MOST = 3
RECV_MOST = 4
META = 128
PIECES = 2
CHUNKS = (1, 1, 1)
GRANT = 20
EPS = 1e-06


VMEM = pltpu.MemorySpace.VMEM
SMEM = pltpu.MemorySpace.SMEM
F32 = jnp.float32
BF16 = jnp.bfloat16


def vmem():
    return pl.BlockSpec(memory_space=VMEM)


def smem():
    return pl.BlockSpec(memory_space=SMEM)


def layer_norm(values, gain):
    center = jnp.mean(values, axis=-1, keepdims=True)
    centred = values - center
    spread = jnp.mean(centred * centred, axis=-1, keepdims=True)
    return centred * lax.rsqrt(spread + EPS) * gain


def unit_rows(values):
    scale = lax.rsqrt(jnp.mean(values * values, axis=-1, keepdims=True) + EPS)
    return values * scale * values.shape[-1] ** (-0.5)


def swap(values, axis, bit):
    size = lax.axis_size(axis)
    return lax.ppermute(values, axis, [(i, i ^ bit) for i in range(size)])


def bits_down(size):
    bits = []
    bit = size // 2
    while bit:
        bits.append(bit)
        bit //= 2
    return bits


def gather_blocks(values, axis):
    blocks, order = [values], [0]
    for bit in bits_down(lax.axis_size(axis)):
        blocks = blocks + [swap(block, axis, bit) for block in blocks]
        order = order + [other ^ bit for other in order]
    return blocks, order


def small(mib):
    return pltpu.CompilerParams(vmem_limit_bytes=mib << 20)


def join_kernel(own_ref, other_ref, out_ref):
    count = own_ref.shape[0]
    out_ref[:count] = own_ref[...]
    out_ref[count:] = other_ref[...]


def join(own, other):
    return pl.pallas_call(
        join_kernel,
        out_shape=jax.ShapeDtypeStruct((2 * own.shape[0],) + own.shape[1:], own.dtype),
        in_specs=[vmem()] * 2,
        out_specs=vmem(),
        compiler_params=small(2),
    )(own, other)


def add_kernel(own_ref, other_ref, out_ref):
    out_ref[...] = own_ref[...] + other_ref[...]


def add(own, other):
    return pl.pallas_call(
        add_kernel,
        out_shape=jax.ShapeDtypeStruct(own.shape, own.dtype),
        in_specs=[vmem()] * 2,
        out_specs=vmem(),
        name="add",
        compiler_params=small(1),
    )(own, other)


def trade_order(size):
    order = [0]
    for bit in bits_down(size):
        order = order + [other ^ bit for other in order]
    return order


def double_stack(values, axis):
    *bits, last = bits_down(lax.axis_size(axis))
    for bit in bits:
        values = join(values, swap(values, axis, bit))
    return values, swap(values, axis, last)


def pick_kernel(pieces, sel_hbm, dest_hbm, pixels_ref, cap_hbm, output_ref, pos_hbm, *refs):
    row_refs = refs[: len(CHUNKS)]
    meta_ref, piece_ref, pos_ref, sel_ref, dest_ref, cap_ref, sems = refs[len(CHUNKS) :]
    first = [
        pltpu.make_async_copy(source, target, sems.at[SEND_MOST + 1 + i])
        for i, (source, target) in enumerate(
            ((sel_hbm, sel_ref), (dest_hbm, dest_ref), (cap_hbm, cap_ref), (pos_hbm, pos_ref))
        )
    ]
    for copy in first:
        copy.start()
    first[0].wait()
    first[1].wait()
    count = jnp.int32(0)
    index = [jnp.int32(0)] * SEND_MOST
    target = [jnp.int32(0)] * SEND_MOST
    for e in range(sel_ref.shape[0]):
        here = sel_ref[e] > 0
        for r in range(SEND_MOST):
            take = here & (count == r)
            index[r] = jnp.where(take, e, index[r])
            target[r] = jnp.where(take, dest_ref[e], target[r])
        count = count + here.astype(jnp.int32)
    length = pos_ref.shape[0]
    copies = []
    for c, chunk in enumerate(CHUNKS):
        for i in range(chunk):
            r = sum(CHUNKS[:c]) + i
            place = row_refs[c].at[pl.ds(i * length, length)]
            copies.append(pltpu.make_async_copy(pixels_ref.at[index[r]], place, sems.at[r]))
    height = piece_ref.shape[0]
    start = pl.multiple_of((lax.axis_index("dp") & (pieces - 1)) * height, height)
    copies.append(
        pltpu.make_async_copy(output_ref.at[pl.ds(start, height)], piece_ref, sems.at[SEND_MOST])
    )
    for copy in copies:
        copy.start()
    first[2].wait()
    captions = cap_ref[...].astype(F32)
    width = captions.shape[1]
    example = lax.broadcasted_iota(jnp.int32, captions.shape, 0)
    lane = lax.broadcasted_iota(jnp.int32, (1, META), 1)
    for r in range(SEND_MOST):
        row = jnp.sum(jnp.where(example == index[r], captions, 0.0), axis=0, keepdims=True)
        live = (count > r).astype(F32)
        extra = jnp.where(lane == 0, live, jnp.where(lane == 1, target[r].astype(F32), 0.0))
        meta_ref[0, r : r + 1, :width] = row.astype(BF16)
        meta_ref[0, r : r + 1, width:] = extra.astype(BF16)
    for copy in copies + first[3:]:
        copy.wait()


def pick(selection, destination, pixels, captions, output_weight, position, pieces):
    _, length, depth = pixels.shape
    fan, width = output_weight.shape
    hbm = pl.BlockSpec(memory_space=pltpu.MemorySpace.HBM)
    *rows, caption_meta, piece, own_position = pl.pallas_call(
        functools.partial(pick_kernel, pieces),
        out_shape=tuple(
            jax.ShapeDtypeStruct((chunk * length, depth), BF16) for chunk in CHUNKS
        )
        + (
            jax.ShapeDtypeStruct((1, SEND_MOST, captions.shape[1] + META), BF16),
            jax.ShapeDtypeStruct((fan // pieces, width), BF16),
            jax.ShapeDtypeStruct(position.shape, BF16),
        ),
        in_specs=[hbm] * 6,
        out_specs=(vmem(),) * (len(CHUNKS) + 3),
        scratch_shapes=[
            SMEM(selection.shape, jnp.int32),
            SMEM(destination.shape, jnp.int32),
            VMEM(captions.shape, BF16),
            pltpu.SemaphoreType.DMA((SEND_MOST + 5,)),
        ],
        name="pick",
        compiler_params=small(2),
    )(*(
        pltpu.with_memory_space_constraint(array, pltpu.MemorySpace.HBM)
        for array in (selection, destination, pixels, captions, output_weight, position)
    ))
    return rows, caption_meta, piece, own_position


def load_kernel(source_ref, out_ref, sem):
    copy = pltpu.make_async_copy(source_ref, out_ref, sem)
    copy.start()
    copy.wait()


def load(array):
    return pl.pallas_call(
        load_kernel,
        out_shape=jax.ShapeDtypeStruct(array.shape, array.dtype),
        in_specs=[pl.BlockSpec(memory_space=pltpu.MemorySpace.HBM)],
        out_specs=vmem(),
        scratch_shapes=[pltpu.SemaphoreType.DMA],
        name="load",
        compiler_params=small(2),
    )(pltpu.with_memory_space_constraint(array, pltpu.MemorySpace.HBM))


def assemble_kernel(*refs):
    out_ref = refs[-1]
    pieces = refs[:-1]
    height = pieces[0].shape[0]
    here = lax.axis_index("dp") & (len(pieces) - 1)
    for j, ref in enumerate(pieces):
        start = pl.multiple_of((here ^ j) * height, height)
        out_ref[pl.ds(start, height), :] = ref[...]


def assemble(pieces):
    height, width = pieces[0].shape
    return pl.pallas_call(
        assemble_kernel,
        out_shape=jax.ShapeDtypeStruct((height * len(pieces), width), BF16),
        in_specs=[vmem()] * len(pieces),
        out_specs=vmem(),
        name="assemble",
        compiler_params=small(2),
    )(*pieces)


def route_kernel(params_ref, first_ref, second_ref, cap_ref, slot_ref, live_ref, line_ref):
    half = first_ref.shape[0]
    rows = jnp.concatenate(
        [ref[j].astype(F32) for ref in (first_ref, second_ref) for j in range(half)], axis=0
    )
    width = cap_ref.shape[1]
    cap_ref[...] = unit_rows(rows[:, :width])
    extra = rows[:, width:]
    live, target = extra[:, 0:1], extra[:, 1:2]
    me = lax.axis_index("dp")
    offset = lax.broadcasted_iota(jnp.int32, (SEND_MOST, 1), 0)
    spot = jnp.concatenate([(me ^ j) * SEND_MOST + offset for j in trade_order(2 * half)], axis=0)
    mine = (live > 0.0) & (target == me.astype(F32))
    mine = jnp.where(mine, 1.0, 0.0)
    count = rows.shape[0]
    square = (count, count)
    same = lax.broadcasted_iota(jnp.int32, square, 0) == lax.broadcasted_iota(jnp.int32, square, 1)
    mine_row = jnp.sum(jnp.where(same, mine, 0.0), axis=0, keepdims=True)
    spot_col = spot.astype(F32)
    spot_row = jnp.sum(jnp.where(same, spot_col, 0.0), axis=0, keepdims=True)
    place = jnp.sum(jnp.where(spot_row < spot_col, mine_row, 0.0), axis=1, keepdims=True)
    lane = lax.broadcasted_iota(jnp.int32, (count, META), 1)
    slot_ref[...] = jnp.where(place == lane.astype(F32), mine, 0.0)
    live_ref[...] = jnp.broadcast_to(live, (count, META))
    row = lax.broadcasted_iota(jnp.int32, line_ref.shape, 0)
    scale = 10.0 * jnp.exp(jnp.full(line_ref.shape, params_ref[0], F32))
    line_ref[...] = jnp.where(row == 0, scale, 2.0 * params_ref[1])


def route(first, second, params):
    count = 2 * first.shape[0] * SEND_MOST
    return pl.pallas_call(
        route_kernel,
        out_shape=(
            jax.ShapeDtypeStruct((count, first.shape[2] - META), F32),
            jax.ShapeDtypeStruct((count, META), F32),
            jax.ShapeDtypeStruct((count, META), F32),
            jax.ShapeDtypeStruct((2, META), F32),
        ),
        in_specs=[smem()] + [vmem()] * 2,
        out_specs=(vmem(),) * 4,
        name="route",
        compiler_params=small(6),
    )(params, first, second)


def attend_kernel(shards, gains_ref, patch_ref, qkv_ref, *refs):
    pixel_refs = refs[:shards]
    position_refs = refs[shards : 2 * shards]
    hidden_ref, context_ref = refs[2 * shards :]
    block = position_refs[0].shape[0]
    length = block * shards
    images = range(pixel_refs[0].shape[0] // block)
    pixels = jnp.concatenate(
        [ref[i * block : (i + 1) * block, :] for i in images for ref in pixel_refs], axis=0
    )
    position = jnp.concatenate([ref[...] for ref in position_refs], axis=0).astype(F32)
    hidden = jnp.dot(pixels, patch_ref[...], preferred_element_type=F32)
    hidden = hidden + jnp.concatenate([position for _ in images], axis=0)
    hidden_ref[...] = hidden
    normed = layer_norm(hidden, gains_ref[0:1, :]).astype(BF16)
    query, key, value = [
        jnp.dot(normed, qkv_ref[t], preferred_element_type=F32).astype(BF16) for t in range(3)
    ]
    query = query * jnp.asarray(HEAD_DIM ** (-0.5), BF16)
    for i in images:
        rows = slice(i * length, (i + 1) * length)
        parts = []
        for h in range(query.shape[1] // HEAD_DIM):
            cols = slice(h * HEAD_DIM, (h + 1) * HEAD_DIM)
            scores = lax.dot_general(
                query[rows, cols],
                key[rows, cols],
                (((1,), (1,)), ((), ())),
                preferred_element_type=F32,
            )
            weights = jnp.exp(scores - jnp.max(scores, axis=-1, keepdims=True))
            weights = weights * (1.0 / jnp.sum(weights, axis=-1, keepdims=True))
            parts.append(
                jnp.dot(weights.astype(BF16), value[rows, cols], preferred_element_type=F32)
            )
        context_ref[rows, :] = jnp.concatenate(parts, axis=1).astype(BF16)


def attend(pixels, positions, gains, patch_weight, qkv):
    shards = len(pixels)
    length = shards * pixels[0].shape[0]
    width = patch_weight.shape[1]
    return pl.pallas_call(
        functools.partial(attend_kernel, shards),
        out_shape=(
            jax.ShapeDtypeStruct((length, width), F32),
            jax.ShapeDtypeStruct((length, qkv.shape[2]), BF16),
        ),
        in_specs=[vmem()] * (3 + 2 * shards),
        out_specs=(vmem(), vmem()),
        compiler_params=small(GRANT),
    )(gains, patch_weight, qkv, *pixels, *positions)


def mix(hidden, order, which, images, context_refs, output_refs):
    shards = len(order)
    length = hidden.shape[0] // images
    block = length // shards
    for j, context_ref, output_ref in zip(which, context_refs, output_refs):
        places = [order.index(order[p] ^ order[j]) for p in range(shards)]
        starts = [i * length + q * block for i in range(images) for q in places]
        context = jnp.concatenate([context_ref[at : at + block, :] for at in starts], axis=0)
        hidden = hidden + jnp.dot(context, output_ref[...], preferred_element_type=F32)
    return hidden


def blend_kernel(order, which, images, hidden_ref, *refs):
    count = len(which)
    hidden = hidden_ref[...]
    refs[-1][...] = mix(hidden, order, which, images, refs[:count], refs[count : 2 * count])


def blend(contexts, order, which, images, outputs, hidden):
    return pl.pallas_call(
        functools.partial(blend_kernel, tuple(order), tuple(which), images),
        out_shape=jax.ShapeDtypeStruct(hidden.shape, F32),
        in_specs=[vmem()] * (1 + 2 * len(which)),
        out_specs=vmem(),
        compiler_params=small(GRANT),
    )(hidden, *(contexts[j] for j in which), *(outputs[j] for j in which))


def expand_kernel(order, which, images, gains_ref, up_ref, hidden_ref, *refs):
    count = len(which)
    sums_ref = refs[2 * count]
    length = hidden_ref.shape[0] // images
    hidden = mix(hidden_ref[...], order, which, images, refs[:count], refs[count : 2 * count])
    normed = layer_norm(hidden, gains_ref[1:2, :]).astype(BF16)
    expanded = jax.nn.gelu(jnp.dot(normed, up_ref[...], preferred_element_type=F32)).astype(BF16)
    expanded = expanded.astype(F32)
    for i in range(images):
        rows = slice(i * length, (i + 1) * length)
        sums_ref[i : i + 1, :] = jnp.sum(hidden[rows], axis=0, keepdims=True)
        sums_ref[images + i : images + i + 1, :] = jnp.sum(expanded[rows], axis=0, keepdims=True)


def expand(contexts, order, which, images, outputs, hidden, gains, up_weight):
    width = hidden.shape[1]
    return pl.pallas_call(
        functools.partial(expand_kernel, tuple(order), tuple(which), images),
        out_shape=jax.ShapeDtypeStruct((2 * images, width), F32),
        in_specs=[vmem()] * (3 + 2 * len(which)),
        out_specs=vmem(),
        compiler_params=small(GRANT),
    )(gains, up_weight, hidden, *(contexts[j] for j in which), *(outputs[j] for j in which))


def reduce_kernel(scale, down_ref, *refs):
    out_ref = refs[-1]
    sums = refs[:-1]
    halves = [ref.shape[0] // 2 for ref in sums]
    units = jnp.concatenate([ref[n:, :] for n, ref in zip(halves, sums)], axis=0) * scale
    residual = jnp.concatenate([ref[:n, :] for n, ref in zip(halves, sums)], axis=0) * scale
    high = units.astype(BF16)
    low = (units - high.astype(F32)).astype(BF16)
    both = jnp.concatenate([high, low], axis=0)
    product = jnp.dot(both, down_ref[...], preferred_element_type=F32)
    count = sum(halves)
    own = (lax.axis_index("mp") == 0).astype(F32)
    out_ref[...] = product[:count] + product[count:] + residual * own


def reduce_units(sums, down_weight, patches):
    return pl.pallas_call(
        functools.partial(reduce_kernel, 1.0 / patches),
        out_shape=jax.ShapeDtypeStruct((SEND_MOST, down_weight.shape[1]), F32),
        in_specs=[vmem()] * (1 + len(sums)),
        out_specs=vmem(),
        name="reduce",
        compiler_params=small(6),
    )(down_weight, *sums)


def finish_kernel(total, gains_ref, weight_ref, cap_ref, slot_ref, live_ref, line_ref, *refs):
    first_ref, second_ref, out_ref, loss_ref = refs
    half = first_ref.shape[0]
    rows = jnp.concatenate(
        [ref[j] for ref in (first_ref, second_ref) for j in range(half)], axis=0
    )
    slot = slot_ref[...]
    pooled = jnp.concatenate(
        [
            jnp.sum(jnp.where(slot[:, k : k + 1] > 0.0, rows, 0.0), axis=0, keepdims=True)
            for k in range(RECV_MOST)
        ],
        axis=0,
    )
    filled = jnp.max(slot, axis=0, keepdims=True)
    used = jnp.concatenate([filled[:, k : k + 1] for k in range(RECV_MOST)], axis=0)
    normed = layer_norm(pooled, gains_ref[2:3, :]).astype(BF16)
    embedded = jnp.dot(normed, weight_ref[...], preferred_element_type=F32)
    embedded = jnp.where(used > 0.0, embedded, 0.0)
    out_ref[...] = embedded
    captions = cap_ref[...]
    images = unit_rows(embedded)
    lane = lax.broadcasted_iota(jnp.int32, slot.shape, 1)
    products = jnp.zeros(slot.shape, F32)
    for k in range(RECV_MOST):
        product = jnp.sum(captions * images[k : k + 1, :], axis=1, keepdims=True)
        products = jnp.where(lane == k, product, products)
    logits = line_ref[0:1, :] * products + line_ref[1:2, :]
    value = jnp.where(slot > 0.0, -logits, logits)
    terms = jnp.maximum(value, 0.0) + jnp.log1p(jnp.exp(-jnp.abs(value)))
    losses = jnp.sum(terms * live_ref[...], axis=0, keepdims=True) * (1.0 / total) * filled
    loss_ref[...] = losses[0, :RECV_MOST]


def finish(first, second, routed, gains, weight, total):
    return pl.pallas_call(
        functools.partial(finish_kernel, total),
        out_shape=(
            jax.ShapeDtypeStruct((RECV_MOST, weight.shape[1]), F32),
            jax.ShapeDtypeStruct((RECV_MOST,), F32),
        ),
        in_specs=[vmem()] * 8,
        out_specs=(vmem(), vmem()),
        name="finish",
        compiler_params=small(8),
    )(gains, weight, *routed, first, second)


def per_device(
    pixels,
    selection,
    destination,
    patch_weight,
    position,
    query_key_value,
    output_weight,
    up_weight,
    down_weight,
    norm_gains,
    embedding_weight,
    caption_vectors,
    loss_params,
):
    devices_dp = lax.axis_size("dp")
    shards = lax.axis_size("mp")
    pieces = count_pieces(devices_dp)
    positions, order = gather_blocks(position, "mp")
    rows, caption_meta, piece, own_position = pick(
        selection, destination, pixels, caption_vectors, output_weight, position, pieces
    )
    positions = [own_position] + positions[1:]
    query_key_value = load(query_key_value)
    pixel_blocks = [gather_blocks(row, "mp")[0] for row in rows]

    parts = [swap(piece, "mp", shards // 2)]
    bit = 1
    while bit < pieces:
        parts = parts + [swap(part, "dp", bit) for part in parts]
        bit *= 2
    outputs = [output_weight, assemble(parts)]
    for bit in bits_down(shards)[1:]:
        outputs = outputs + [swap(block, "mp", bit) for block in outputs]

    routed = route(*double_stack(caption_meta, "dp"), loss_params)

    sums = []
    for r, images in enumerate(CHUNKS):
        hidden, context = attend(
            pixel_blocks[r], positions, norm_gains, patch_weight, query_key_value
        )
        contexts, _ = gather_blocks(context, "mp")
        which = list(range(shards))
        if r == len(CHUNKS) - 1:
            hidden = blend(contexts, order, which[:-1], images, outputs, hidden)
            which = which[-1:]
        sums.append(expand(contexts, order, which, images, outputs, hidden, norm_gains, up_weight))
    pooled = reduce_units(sums, down_weight, position.shape[0] * shards)
    for bit in reversed(bits_down(shards)):
        pooled = add(pooled, swap(pooled, "mp", bit))
    first, second = double_stack(pooled[None], "dp")
    return finish(
        first, second, routed, norm_gains, embedding_weight, float(devices_dp * SEL_DEV)
    )


def count_pieces(devices_dp):
    pieces = 1
    while pieces < PIECES and 2 * pieces <= devices_dp:
        pieces *= 2
    return pieces


def solution(mesh):
    in_specs = (
        P("dp", "mp", None),
        P("dp"),
        P("dp"),
        P(),
        P("mp", None),
        P(None, None, "mp"),
        P("mp", None),
        P(None, "mp"),
        P("mp", None),
        P(),
        P(),
        P("dp", None),
        P(),
    )
    out_specs = (P("dp", None), P("dp"))

    return jax.shard_map(
        per_device, mesh=mesh, in_specs=in_specs, out_specs=out_specs, check_vma=False
    )
```
